128 devices in a mesh: wa: 32 (over x, z_hi, y), ch: 4 (over z_lo, core).
Axes of the slice: x: 4, y: 4, z: 4 (z_hi: 2, z_lo: 2; z = z_hi * 2 + z_lo), core: 2. Of those that a mesh axis runs over, the one named last changes fastest.
Arguments:
- grid_cells: int32 [2, 65536], P(None, ('wa', 'ch')), may hold values from -4096 to 4095
- visibilities: float32 [2, 65536], P(None, ('wa', 'ch')), may hold values from -6 to 6
- weights: float32 [65536], P(('wa', 'ch')), may hold values from 0.25 to 4
- layer_index: int32 [65536], P(('wa', 'ch')), may hold values from 0 to 31, as said below
- group_index: int32 [65536], P(('wa', 'ch')), may hold values from 0 to 3, as said below
- plane_depths: float32 [32], P('wa'), may hold values from -1000 to 1000
- sky_model: float32 [4, 512, 4096], P('ch', 'wa'), may hold values from -6 to 6
Outputs:
- residual: float32 [4, 512, 4096], P('ch', 'wa')
The draws below stay inside these ranges and needn't reach their ends.
Inputs may be any that keep to these rules, and one draw needn't show every extreme that they name: `layer_index`: among the 512 visibilities of one device, at most 8 have the same layer and the same group; one layer and group has exactly 8 on every device. `group_index`: drawn together with layer_index.
All inputs are finite; a program needn't handle non-finite values.
Results may differ from the reference program's by a relative error of at most 0.0026.
Values sent between devices are 32-bit elements; how exact they have to be, the bound alone decides.
A program may use at most 128 MiB of HBM per device.

```python
import math
import jax
import jax.numpy as jnp
from jax import lax

GRID = 8192
VIS_DEV = 512
ROWS_DEV = 16
FACET_COLS = 4096
LAYERS = 32
GROUPS = 4
VIS = 65536
CAP = 8
FACET_ROWS = 512
N_WA = 32
N_CH = 4


def route_draw(key):
    blocks = VIS // VIS_DEV
    dest_count = LAYERS * GROUPS
    favoured = jax.random.randint(jax.random.fold_in(key, 11), (), 0, dest_count)

    def one_block(block_number):
        block_key = jax.random.fold_in(jax.random.fold_in(key, 13), block_number)
        order_key, share_key, shuffle_key = jax.random.split(block_key, 3)
        sequence = jax.random.permutation(order_key, dest_count).astype(jnp.int32)
        position_found = jnp.argmax(sequence == favoured)
        leading = sequence[0]
        sequence = sequence.at[position_found].set(leading).at[0].set(favoured)
        shares = jax.random.randint(share_key, (dest_count // 2,), 0, CAP + 1).at[0].set(CAP)
        paired = jnp.stack([shares, CAP - shares], 1).reshape(dest_count)
        counts = jnp.zeros((dest_count,), jnp.int32).at[sequence].set(paired.astype(jnp.int32))
        boundaries = jnp.cumsum(counts)
        position = jnp.arange(VIS_DEV, dtype=jnp.int32)
        destination = jnp.sum((position[:, None] >= boundaries[None, :]).astype(jnp.int32), 1)
        return jax.random.permutation(shuffle_key, destination)
    every = jax.vmap(one_block)(jnp.arange(blocks, dtype=jnp.int32))
    return every.reshape(VIS).astype(jnp.int32)


def draw_layer_index(key, part):
    return (route_draw(jax.random.fold_in(key, 7)) // GROUPS).astype(jnp.int32)


def draw_group_index(key, part):
    return (route_draw(jax.random.fold_in(key, 7)) % GROUPS).astype(jnp.int32)


def touch_ends(entries, rng, least, top_value):
    longest = entries.shape.index(max(entries.shape))
    spots = []
    for shift in (0, 1):
        where = [jax.random.randint(jax.random.fold_in(rng, axis), (), 0, length) for axis, length in enumerate(entries.shape)]
        where[longest] = (where[longest] + shift) % entries.shape[longest]
        spots.append(tuple(where))
    return entries.at[spots[0]].set(least).at[spots[1]].set(top_value)


def level_of(key, dims, shards, least, largest):
    loudness, own = 1.0, jax.random.fold_in(key, 6)
    for axis_at, blocks in shards:
        draws = jnp.exp(jax.random.uniform(jax.random.fold_in(own, axis_at), (blocks,), jnp.float32, least / len(shards), largest / len(shards)))
        loudness = loudness * jnp.repeat(draws, dims[axis_at] // blocks).reshape([-1 if axis == axis_at else 1 for axis in range(len(dims))])
    return loudness


def centred(own_key, shape, width, reach, cuts=(), kind=jnp.bfloat16):
    entries = width * jax.random.normal(own_key, shape, jnp.float32)
    if cuts:
        entries = entries * level_of(own_key, shape, cuts, -0.22, 0.18)
    return jnp.clip(entries, -reach, reach).astype(kind)


def setup_inputs(seed: int = 0) -> dict:
    arg_keys = jax.random.split(jax.random.key(seed), 8)
    grid_cells = touch_ends(jax.random.randint(arg_keys[0], (2, VIS), -(GRID // 2), GRID // 2), jax.random.fold_in(arg_keys[0], 1), -(GRID // 2), (GRID // 2) - 1).astype(jnp.int32)
    visibilities = centred(arg_keys[1], (2, VIS), 1.0, 6.0, ((1, 128),), jnp.float32)
    weights = jnp.clip(jnp.exp(math.log(4.0) - 2.7725887 * jax.random.uniform(arg_keys[2], (VIS,), jnp.float32) ** level_of(arg_keys[2], (VIS,), ((0, 128),), -0.2, 0.2)), 0.25, 4.0)
    layer_index = draw_layer_index(jax.random.fold_in(arg_keys[7], 71), 0)
    group_index = draw_group_index(jax.random.fold_in(arg_keys[7], 71), 0)
    plane_depths = jnp.clip(jax.random.uniform(arg_keys[5], (LAYERS,), jnp.float32, -1000.0, 1000.0) * level_of(arg_keys[5], (LAYERS,), ((0, 32),), -0.4, 0.0), -1000.0, 1000.0)
    sky_model = centred(arg_keys[6], (GROUPS, FACET_ROWS, FACET_COLS), 1.0, 6.0, ((0, 4), (1, 32)), jnp.float32)
    return dict(grid_cells=grid_cells, visibilities=visibilities, weights=weights, layer_index=layer_index, group_index=group_index, plane_depths=plane_depths, sky_model=sky_model)


def phase_table(left, right, grid_size):
    product = jnp.mod(left[:, None] * right[None, :], grid_size)
    return product.astype(jnp.float32) * (2.0 * math.pi / grid_size)

def column_factor(real_part, imag_part, weight, column_cells, columns, grid_size):
    pixels = jnp.arange(columns, dtype=jnp.int32) - columns // 2 + grid_size // 8
    angles = phase_table(column_cells, pixels, grid_size)
    weighted_real = weight * real_part
    weighted_imag = weight * imag_part
    cosines = jnp.cos(angles)
    sine_values = jnp.sin(angles)
    column_real = (weighted_real[:, None] * cosines - weighted_imag[:, None] * sine_values).astype(jnp.bfloat16)
    column_imag = (weighted_real[:, None] * sine_values + weighted_imag[:, None] * cosines).astype(jnp.bfloat16)
    return jnp.concatenate([column_real, column_imag], 0)

def row_factor(row_cells, row_start, row_count, total_rows, grid_size):
    pixels = row_start + jnp.arange(row_count, dtype=jnp.int32) - total_rows // 2 + grid_size // 8
    angles = phase_table(pixels, row_cells, grid_size)
    real_part = jnp.cos(angles).astype(jnp.bfloat16)
    imag_part = jnp.sin(angles).astype(jnp.bfloat16)
    upper_half = jnp.concatenate([real_part, -imag_part], 1)
    lower_half = jnp.concatenate([imag_part, real_part], 1)
    return jnp.concatenate([upper_half, lower_half], 0)

def layer_image(row_factors, column_factors, w_value, row_start, row_count, total_rows, columns, grid_size):
    product = jnp.dot(row_factors, column_factors, preferred_element_type=jnp.float32)
    real_sum = product[:row_count]
    imag_sum = product[row_count:]
    row_pixels = row_start + jnp.arange(row_count, dtype=jnp.int32) - total_rows // 2 + grid_size // 8
    column_pixels = jnp.arange(columns, dtype=jnp.int32) - columns // 2 + grid_size // 8
    row_cosine = 0.8 * row_pixels.astype(jnp.float32) / grid_size
    column_cosine = 0.8 * column_pixels.astype(jnp.float32) / grid_size
    depth_term = jnp.sqrt(1.0 - row_cosine[:, None] ** 2 - column_cosine[None, :] ** 2) - 1.0
    screen = 2.0 * math.pi * w_value * depth_term
    return jnp.cos(screen) * real_sum - jnp.sin(screen) * imag_sum

def reference(grid_cells, visibilities, weights, layer_index, group_index, plane_depths, sky_model):
    dest_count = N_WA * N_CH
    slot_count = CAP * N_WA * N_CH
    total_rows = ROWS_DEV * N_WA
    columns = FACET_COLS
    target = (layer_index * N_CH + group_index).astype(jnp.int32)
    sorting = jnp.argsort(target, stable=True)
    counts = jnp.bincount(target, length=dest_count).astype(jnp.int32)
    starts = (jnp.cumsum(counts) - counts).astype(jnp.int32)
    payload = jnp.stack([visibilities[0], visibilities[1], weights], 0)[:, sorting]
    payload = jnp.concatenate([payload, jnp.zeros((3, slot_count), payload.dtype)], 1)
    cells = grid_cells[:, sorting].astype(jnp.int32)
    cells = jnp.concatenate([cells, jnp.zeros((2, slot_count), jnp.int32)], 1)

    def add_dest(dirty_all, dest_number):
        offset_start = starts[dest_number]
        dest_data = lax.dynamic_slice_in_dim(payload, offset_start, slot_count, 1)
        dest_cells = lax.dynamic_slice_in_dim(cells, offset_start, slot_count, 1)
        live_mask = (jnp.arange(slot_count, dtype=jnp.int32) < counts[dest_number]).astype(dest_data.dtype)
        weight = dest_data[2] * live_mask
        column_factors = column_factor(dest_data[0], dest_data[1], weight, dest_cells[1], columns, GRID)
        row_factors = row_factor(dest_cells[0], jnp.int32(0), total_rows, total_rows, GRID)
        contribution = layer_image(row_factors, column_factors, plane_depths[dest_number // N_CH], jnp.int32(0), total_rows, total_rows, columns, GRID)
        target_group = dest_number % N_CH
        return (dirty_all.at[target_group].add(contribution), None)
    dirty_all, _ = lax.scan(add_dest, jnp.zeros((N_CH, total_rows, columns), jnp.float32), jnp.arange(dest_count, dtype=jnp.int32))
    member = (group_index[None, :] == jnp.arange(N_CH, dtype=jnp.int32)[:, None]).astype(jnp.float32)
    noise_power = lax.optimization_barrier(jnp.sum(member * (weights * weights)[None, :], 1))
    return dirty_all * lax.rsqrt(noise_power)[:, None, None] - sky_model
```

```python
import functools
import math

import jax
import jax.numpy as jnp
from jax import lax
from jax.experimental import pallas as pl
from jax.experimental.pallas import tpu as pltpu
from jax.sharding import PartitionSpec as P

F32 = jnp.float32
BF16 = jnp.bfloat16
I32 = jnp.int32

GRID = 8192
LAYERS = 32
GROUPS = 4
SOURCES = 128
CAP = 8
LANES = 128
VIS_DEV = 512
ROWS = 16
COLS = 4096
BLOCKS = COLS // 256
MSG = 10

SIN_C = (4.442882919124344, -7.308245686509099, 3.6063542184331383, -0.8461116503741475, 0.10982451642439378)
COS_C = (1.4142134962552289, -6.978850948563853, 5.7394603769076955, -1.8835579059892091, 0.31068802753070307)


def horner(g, coefs):
    total = coefs[-1] * g + coefs[-2]
    for c in coefs[-3::-1]:
        total = total * g + c
    return total


def sincos_turns(f):
    g = f * f
    s = horner(g, SIN_C) * f
    c = horner(g, COS_C)
    return 1.0 - s * s, s * c


def sincos_phase(p):
    q = ((p + GRID) & (2 * GRID - 1)) - GRID
    return sincos_turns(q.astype(F32) * (1.0 / (2 * GRID)))


def cmul(a, b):
    return a[0] * b[0] - a[1] * b[1], a[0] * b[1] + a[1] * b[0]


def route_kernel(cells, vis, weights, layer, group, depth, out):
    w = weights[...]
    target_row = (layer[...] * GROUPS + group[...]).astype(F32)
    blocks = VIS_DEV // LANES
    lane = lax.broadcasted_iota(I32, (LANES, LANES), 1)
    sub = lax.broadcasted_iota(I32, (LANES, LANES), 0)
    slots = []
    for b in range(blocks):
        mine = target_row[:, b * LANES : (b + 1) * LANES]
        across = jnp.broadcast_to(mine, (LANES, LANES)).T
        hits = jnp.where((across == mine) & (lane < sub), 1.0, 0.0)
        for other in range(b):
            theirs = target_row[:, other * LANES : (other + 1) * LANES]
            hits += jnp.where(across == theirs, 1.0, 0.0)
        rank = jnp.sum(hits, axis=1, keepdims=True).astype(I32)
        t = across.astype(I32)
        slots.append((t & 3) * (LAYERS * CAP) + (t >> 2) * CAP + rank)
    zero = jnp.zeros((1, VIS_DEV), F32)
    values = jnp.concatenate(
        [
            w * vis[0:1, :],
            w * vis[1:2, :],
            cells[0:1, :].astype(F32),
            cells[1:2, :].astype(F32),
            zero,
            zero,
            zero,
            zero,
        ],
        0,
    )
    high = values.astype(BF16)
    rest = values - high.astype(F32)
    middle = rest.astype(BF16)
    low = (rest - middle.astype(F32)).astype(BF16)
    for group_number in range(GROUPS):
        for half in range(2):
            first = (group_number * 2 + half) * LANES
            picks = jnp.concatenate(
                [jnp.where(slots[b] == lane + first, 1.0, 0.0).astype(BF16) for b in range(blocks)], 0
            )
            total = jnp.dot(high, picks, preferred_element_type=F32)
            total += jnp.dot(middle, picks, preferred_element_type=F32)
            total += jnp.dot(low, picks, preferred_element_type=F32)
            out[group_number, half * 4 : half * 4 + 4, :] = total[0:4]
        power = jnp.sum(jnp.where(group[...] == group_number, w * w, 0.0), axis=1, keepdims=True)
        out[group_number, 8:9, :] = jnp.zeros((1, LANES), F32) + depth[0]
        out[group_number, 9:10, :] = jnp.zeros((1, LANES), F32) + power


def image_kernel(first_row, got, sky, out, vals, wtab, ltab, ntab, c16, dterm, acc, ximg, lhs_a, rhs_a, lhs_b, rhs_b):
    row0 = first_row[0]
    for half in range(2):
        for v in range(4):
            vals[v, half * LANES : (half + 1) * LANES, :] = got[:, half * 4 + v, :].T
    sub = lax.broadcasted_iota(I32, (8, LANES), 0)
    lane = lax.broadcasted_iota(I32, (8, LANES), 1)
    for sl in range(2):
        rows = (row0 + 768) + (8 + sub if sl == 0 else 7 - sub)
        l = 0.8 * rows.astype(F32) / GRID
        for sn in range(2):
            for c0 in range(BLOCKS):
                cols = 256 * c0 - 1024 + (128 + lane if sn == 0 else 127 - lane)
                m = 0.8 * cols.astype(F32) / GRID
                q = l * l + m * m
                t = (c0 * 2 + sl) * 2 + sn
                dterm[t * 8 : t * 8 + 8, :] = -q / (1.0 + jnp.sqrt(1.0 - q))
    acc[...] = jnp.zeros_like(acc)

    def tables(jc, carry):
        base = pl.multiple_of(jc * 32, 32)
        zr = vals[0, pl.ds(base, 32), :]
        zi = vals[1, pl.ds(base, 32), :]
        u = vals[2, pl.ds(base, 32), :].astype(I32)
        v = vals[3, pl.ds(base, 32), :].astype(I32)

        def put(ref, per_layer, q, x):
            for i in range(4):
                at = pl.multiple_of((jc * 4 + i) * per_layer * 8, 8) + q * 8
                ref[pl.ds(at, 8), :] = x[i * 8 : i * 8 + 8]

        w = cmul((zr, zi), sincos_phase((2 * row0 + 1551) * u - 1793 * v))
        step = sincos_phase(512 * v)
        for c0 in range(BLOCKS):
            put(wtab, 32, c0 * 2, w[0])
            put(wtab, 32, c0 * 2 + 1, w[1])
            if c0 + 1 < BLOCKS:
                w = cmul(w, step)
        half_step = sincos_phase(u)
        step = cmul(half_step, half_step)
        e = half_step
        for n in range(8):
            put(ltab, 16, n, e[0])
            put(ltab, 16, 8 + n, e[1])
            if n < 7:
                e = cmul(e, step)
        half_step = sincos_phase(v)
        step = cmul(half_step, half_step)
        e = half_step
        for n in range(16):
            put(ntab, 64, n, e[0])
            put(ntab, 64, 15 - n + 16, e[0])
            put(ntab, 64, n + 32, e[1])
            put(ntab, 64, 15 - n + 48, -e[1])
            if n < 15:
                e = cmul(e, step)
        c16[pl.ds(base, 32), :] = 2.0 * sincos_phase(32 * v)[0]
        return carry

    lax.fori_loop(0, LAYERS // 4, tables, 0)

    def expand(j, lhs, rhs):
        for s in range(8):
            ks = slice(s * LANES, (s + 1) * LANES)
            lbase = ltab[pl.ds(j * 128 + s, 16, stride=8), :]
            for q in range(32):
                row = wtab[pl.ds(j * 256 + q * 8 + s, 1), :]
                lhs[q * 16 : q * 16 + 16, ks] = (lbase * row).astype(BF16)
            c2 = c16[pl.ds(j * 8 + s, 1), :]
            for part in range(2):
                now = ntab[pl.ds(j * 512 + part * 256 + s, 16, stride=8), :]
                last = ntab[pl.ds(j * 512 + part * 256 + 128 + s, 16, stride=8), :]
                for b in range(8):
                    rhs[part * 128 + b * 16 : part * 128 + b * 16 + 16, ks] = now.astype(BF16)
                    if b < 7:
                        now, last = c2 * now - last, now

    def image(j, lhs, rhs):
        ximg[...] = lax.dot_general(
            lhs[...], rhs[...], (((1,), (1,)), ((), ())), preferred_element_type=F32
        )
        depth = got[pl.ds(j * GROUPS, 1), 8, :]
        for c0 in range(BLOCKS):
            parts = []
            for ri in range(2):
                at = (c0 * 2 + ri) * 16
                cc = ximg[at : at + 8, 0:LANES]
                cs = ximg[at : at + 8, LANES:]
                sc = ximg[at + 8 : at + 16, 0:LANES]
                ss = ximg[at + 8 : at + 16, LANES:]
                parts.append((cc - ss, cc + ss, sc + cs, sc - cs))
            (ra, rb, rp, rm), (ia, ib, ip, im) = parts
            pixels = ((ra - ip, ia + rp), (rb - im, ib + rm), (rb + im, ib - rm), (ra + ip, ia - rp))
            for k, (pr, pi) in enumerate(pixels):
                at = (c0 * 4 + k) * 8
                t = depth * dterm[at : at + 8, :]
                cos, sin = sincos_turns(t - jnp.round(t))
                acc[at : at + 8, :] += cos * pr - sin * pi

    expand(0, lhs_a, rhs_a)

    def pair(jj, carry):
        expand(2 * jj + 1, lhs_b, rhs_b)
        image(2 * jj, lhs_a, rhs_a)
        expand(jnp.minimum(2 * jj + 2, LAYERS - 1), lhs_a, rhs_a)
        image(2 * jj + 1, lhs_b, rhs_b)
        return carry

    lax.fori_loop(0, LAYERS // 2, pair, 0)

    noise = jnp.sum(got[:, 9, :], axis=0, keepdims=True)
    scale = lax.rsqrt(noise)
    back_lane = (LANES - 1) - lane
    for c0 in range(BLOCKS):
        for k in range(4):
            at = (c0 * 4 + k) * 8
            tile = acc[at : at + 8, :] * scale
            if k % 2 == 1:
                tile = jnp.take_along_axis(tile, back_lane, axis=1, mode="promise_in_bounds")
            cols = slice(c0 * 256 + (128 if k % 2 == 0 else 0), c0 * 256 + (256 if k % 2 == 0 else 128))
            if k < 2:
                out[8:16, cols] = tile - sky[8:16, cols]
            else:
                for n in range(8):
                    out[7 - n : 8 - n, cols] = tile[n : n + 1] - sky[7 - n : 8 - n, cols]


def on_device(grid_cells, visibilities, weights, layer_index, group_index, plane_depths, sky_model):
    vmem = pl.BlockSpec(memory_space=pltpu.VMEM)
    smem = pl.BlockSpec(memory_space=pltpu.SMEM)
    blocks = pl.pallas_call(
        route_kernel,
        out_shape=jax.ShapeDtypeStruct((GROUPS, MSG, LANES), F32),
        in_specs=[vmem] * 5 + [smem],
        out_specs=vmem,
        name="route",
    )(
        grid_cells,
        visibilities,
        weights.reshape(1, VIS_DEV),
        layer_index.reshape(1, VIS_DEV),
        group_index.reshape(1, VIS_DEV),
        plane_depths,
    )
    mine = lax.all_to_all(blocks, "ch", split_axis=0, concat_axis=0, tiled=True)
    got = lax.all_gather(mine, "wa", axis=0, tiled=True)
    first_row = (lax.axis_index("wa") * ROWS).astype(I32).reshape(1)
    sky = sky_model[0]
    residual = pl.pallas_call(
        image_kernel,
        out_shape=jax.ShapeDtypeStruct((ROWS, COLS), F32),
        in_specs=[smem, vmem, vmem],
        out_specs=vmem,
        scratch_shapes=[
            pltpu.VMEM((4, LAYERS * CAP, LANES), F32),
            pltpu.VMEM((LAYERS * 32 * 8, LANES), F32),
            pltpu.VMEM((LAYERS * 16 * 8, LANES), F32),
            pltpu.VMEM((LAYERS * 64 * 8, LANES), F32),
            pltpu.VMEM((LAYERS * 8, LANES), F32),
            pltpu.VMEM((64 * 8, LANES), F32),
            pltpu.VMEM((64 * 8, LANES), F32),
            pltpu.VMEM((512, 256), F32),
            pltpu.VMEM((512, 1024), BF16),
            pltpu.VMEM((256, 1024), BF16),
            pltpu.VMEM((512, 1024), BF16),
            pltpu.VMEM((256, 1024), BF16),
        ],
        compiler_params=pltpu.CompilerParams(vmem_limit_bytes=60 * 1024 * 1024),
        name="image",
    )(first_row, got, sky)
    return residual[None]


def solution(mesh):
    both = ("wa", "ch")
    return jax.shard_map(
        on_device,
        mesh=mesh,
        in_specs=(
            P(None, both),
            P(None, both),
            P(both),
            P(both),
            P(both),
            P("wa"),
            P("ch", "wa", None),
        ),
        out_specs=P("ch", "wa", None),
        check_vma=False,
    )
```

```python
import functools
import math

import jax
import jax.numpy as jnp
from jax import lax
from jax.experimental import pallas as pl
from jax.experimental.pallas import tpu as pltpu
from jax.sharding import PartitionSpec as P

F32 = jnp.float32
BF16 = jnp.bfloat16
I32 = jnp.int32

GRID = 8192
LAYERS = 32
GROUPS = 4
SOURCES = 128
CAP = 8
LANES = 128
VIS_DEV = 512
ROWS = 16
COLS = 4096
BLOCKS = COLS // 256
MSG = 10

SIN_C = (4.442882919124344, -7.308245686509099, 3.6063542184331383, -0.8461116503741475, 0.10982451642439378)
COS_C = (1.4142134962552289, -6.978850948563853, 5.7394603769076955, -1.8835579059892091, 0.31068802753070307)


def horner(g, coefs):
    total = coefs[-1] * g + coefs[-2]
    for c in coefs[-3::-1]:
        total = total * g + c
    return total


def sincos_turns(f):
    g = f * f
    s = horner(g, SIN_C) * f
    c = horner(g, COS_C)
    return 1.0 - s * s, s * c


def sincos_phase(p):
    q = ((p + GRID) & (2 * GRID - 1)) - GRID
    return sincos_turns(q.astype(F32) * (1.0 / (2 * GRID)))


def cmul(a, b):
    return a[0] * b[0] - a[1] * b[1], a[0] * b[1] + a[1] * b[0]


def fill_blocks(cells, vis, weights, layer, group, depth, out):
    w = weights[...]
    target_row = (layer[...] * GROUPS + group[...]).astype(F32)
    blocks = VIS_DEV // LANES
    lane = lax.broadcasted_iota(I32, (LANES, LANES), 1)
    sub = lax.broadcasted_iota(I32, (LANES, LANES), 0)
    slots = []
    for b in range(blocks):
        mine = target_row[:, b * LANES : (b + 1) * LANES]
        across = jnp.broadcast_to(mine, (LANES, LANES)).T
        hits = jnp.where((across == mine) & (lane < sub), 1.0, 0.0)
        for other in range(b):
            theirs = target_row[:, other * LANES : (other + 1) * LANES]
            hits += jnp.where(across == theirs, 1.0, 0.0)
        rank = jnp.sum(hits, axis=1, keepdims=True).astype(I32)
        t = across.astype(I32)
        slots.append((t & 3) * (LAYERS * CAP) + (t >> 2) * CAP + rank)
    zero = jnp.zeros((1, VIS_DEV), F32)
    values = jnp.concatenate(
        [
            w * vis[0:1, :],
            w * vis[1:2, :],
            cells[0:1, :].astype(F32),
            cells[1:2, :].astype(F32),
            zero,
            zero,
            zero,
            zero,
        ],
        0,
    )
    high = values.astype(BF16)
    rest = values - high.astype(F32)
    middle = rest.astype(BF16)
    low = (rest - middle.astype(F32)).astype(BF16)
    for group_number in range(GROUPS):
        for half in range(2):
            first = (group_number * 2 + half) * LANES
            picks = jnp.concatenate(
                [jnp.where(slots[b] == lane + first, 1.0, 0.0).astype(BF16) for b in range(blocks)], 0
            )
            total = jnp.dot(high, picks, preferred_element_type=F32)
            total += jnp.dot(middle, picks, preferred_element_type=F32)
            total += jnp.dot(low, picks, preferred_element_type=F32)
            out[group_number, half * 4 : half * 4 + 4, :] = total[0:4]
        power = jnp.sum(jnp.where(group[...] == group_number, w * w, 0.0), axis=1, keepdims=True)
        out[group_number, 8:9, :] = jnp.zeros((1, LANES), F32) + depth[0]
        out[group_number, 9:10, :] = jnp.zeros((1, LANES), F32) + power


def exchange_kernel(mult, cells, vis, weights, layer, group, depth, vals, misc, blocks, recv, send_sem, recv_sem):
    wa = lax.axis_index("wa")
    ch = lax.axis_index("ch")
    me = wa * GROUPS + ch
    barrier = pltpu.get_barrier_semaphore()

    def device(d):
        other = lax.rem(me + lax.rem(d * mult, SOURCES), SOURCES)
        return other // GROUPS, lax.rem(other, GROUPS)

    def greet(d, carry):
        pl.semaphore_signal(barrier, inc=1, device_id=device(d), device_id_type=pl.DeviceIdType.MESH)
        return carry

    lax.fori_loop(1, SOURCES, greet, 0)
    fill_blocks(cells, vis, weights, layer, group, depth, blocks)
    pl.semaphore_wait(barrier, SOURCES - 1)

    def send(d, carry):
        to = device(d)
        pltpu.make_async_remote_copy(
            src_ref=blocks.at[to[1]],
            dst_ref=recv.at[me],
            send_sem=send_sem,
            recv_sem=recv_sem,
            device_id=to,
            device_id_type=pl.DeviceIdType.MESH,
        ).start()
        return carry

    lax.fori_loop(1, SOURCES, send, 0)
    recv[me] = blocks[ch]
    rest = recv.at[pl.ds(0, SOURCES - 1)]
    pltpu.make_async_copy(rest, rest, recv_sem).wait()
    for half in range(2):
        for v in range(4):
            vals[v, half * LANES : (half + 1) * LANES, :] = recv[:, half * 4 + v, :].T
    misc[0] = recv[:, 8, :]
    misc[1] = recv[:, 9, :]
    pltpu.make_async_copy(rest, rest, send_sem).wait()


def image_kernel(first_row, vals, misc, sky, out, wtab, ltab, ntab, c16, dterm, acc, ximg, lhs_a, rhs_a, lhs_b, rhs_b):
    row0 = first_row[0]
    sub = lax.broadcasted_iota(I32, (8, LANES), 0)
    lane = lax.broadcasted_iota(I32, (8, LANES), 1)
    for sl in range(2):
        rows = (row0 + 768) + (8 + sub if sl == 0 else 7 - sub)
        l = 0.8 * rows.astype(F32) / GRID
        for sn in range(2):
            for c0 in range(BLOCKS):
                cols = 256 * c0 - 1024 + (128 + lane if sn == 0 else 127 - lane)
                m = 0.8 * cols.astype(F32) / GRID
                q = l * l + m * m
                t = (c0 * 2 + sl) * 2 + sn
                dterm[t * 8 : t * 8 + 8, :] = -q / (1.0 + jnp.sqrt(1.0 - q))
    acc[...] = jnp.zeros_like(acc)

    def tables(jc, carry):
        base = pl.multiple_of(jc * 32, 32)
        zr = vals[0, pl.ds(base, 32), :]
        zi = vals[1, pl.ds(base, 32), :]
        u = vals[2, pl.ds(base, 32), :].astype(I32)
        v = vals[3, pl.ds(base, 32), :].astype(I32)

        def put(ref, per_layer, q, x):
            for i in range(4):
                at = pl.multiple_of((jc * 4 + i) * per_layer * 8, 8) + q * 8
                ref[pl.ds(at, 8), :] = x[i * 8 : i * 8 + 8]

        w = cmul((zr, zi), sincos_phase((2 * row0 + 1551) * u - 1793 * v))
        step = sincos_phase(512 * v)
        for c0 in range(BLOCKS):
            put(wtab, 32, c0 * 2, w[0])
            put(wtab, 32, c0 * 2 + 1, w[1])
            if c0 + 1 < BLOCKS:
                w = cmul(w, step)
        half_step = sincos_phase(u)
        step = cmul(half_step, half_step)
        e = half_step
        for n in range(8):
            put(ltab, 16, n, e[0])
            put(ltab, 16, 8 + n, e[1])
            if n < 7:
                e = cmul(e, step)
        half_step = sincos_phase(v)
        step = cmul(half_step, half_step)
        e = half_step
        for n in range(16):
            put(ntab, 64, n, e[0])
            put(ntab, 64, 15 - n + 16, e[0])
            put(ntab, 64, n + 32, e[1])
            put(ntab, 64, 15 - n + 48, -e[1])
            if n < 15:
                e = cmul(e, step)
        c16[pl.ds(base, 32), :] = 2.0 * sincos_phase(32 * v)[0]
        return carry

    lax.fori_loop(0, LAYERS // 4, tables, 0)

    def expand(j, lhs, rhs):
        for s in range(8):
            ks = slice(s * LANES, (s + 1) * LANES)
            lbase = ltab[pl.ds(j * 128 + s, 16, stride=8), :]
            for q in range(32):
                row = wtab[pl.ds(j * 256 + q * 8 + s, 1), :]
                lhs[q * 16 : q * 16 + 16, ks] = (lbase * row).astype(BF16)
            c2 = c16[pl.ds(j * 8 + s, 1), :]
            for part in range(2):
                now = ntab[pl.ds(j * 512 + part * 256 + s, 16, stride=8), :]
                last = ntab[pl.ds(j * 512 + part * 256 + 128 + s, 16, stride=8), :]
                for b in range(8):
                    rhs[part * 128 + b * 16 : part * 128 + b * 16 + 16, ks] = now.astype(BF16)
                    if b < 7:
                        now, last = c2 * now - last, now

    def image(j, lhs, rhs):
        ximg[...] = lax.dot_general(
            lhs[...], rhs[...], (((1,), (1,)), ((), ())), preferred_element_type=F32
        )
        depth = misc[0, pl.ds(j * GROUPS, 1), :]
        for c0 in range(BLOCKS):
            parts = []
            for ri in range(2):
                at = (c0 * 2 + ri) * 16
                cc = ximg[at : at + 8, 0:LANES]
                cs = ximg[at : at + 8, LANES:]
                sc = ximg[at + 8 : at + 16, 0:LANES]
                ss = ximg[at + 8 : at + 16, LANES:]
                parts.append((cc - ss, cc + ss, sc + cs, sc - cs))
            (ra, rb, rp, rm), (ia, ib, ip, im) = parts
            pixels = ((ra - ip, ia + rp), (rb - im, ib + rm), (rb + im, ib - rm), (ra + ip, ia - rp))
            for k, (pr, pi) in enumerate(pixels):
                at = (c0 * 4 + k) * 8
                t = depth * dterm[at : at + 8, :]
                cos, sin = sincos_turns(t - jnp.round(t))
                acc[at : at + 8, :] += cos * pr - sin * pi

    expand(0, lhs_a, rhs_a)

    def pair(jj, carry):
        expand(2 * jj + 1, lhs_b, rhs_b)
        image(2 * jj, lhs_a, rhs_a)
        expand(jnp.minimum(2 * jj + 2, LAYERS - 1), lhs_a, rhs_a)
        image(2 * jj + 1, lhs_b, rhs_b)
        return carry

    lax.fori_loop(0, LAYERS // 2, pair, 0)

    noise = jnp.sum(misc[1], axis=0, keepdims=True)
    scale = lax.rsqrt(noise)
    back_lane = (LANES - 1) - lane
    for c0 in range(BLOCKS):
        for k in range(4):
            at = (c0 * 4 + k) * 8
            tile = acc[at : at + 8, :] * scale
            if k % 2 == 1:
                tile = jnp.take_along_axis(tile, back_lane, axis=1, mode="promise_in_bounds")
            cols = slice(c0 * 256 + (128 if k % 2 == 0 else 0), c0 * 256 + (256 if k % 2 == 0 else 128))
            if k < 2:
                out[8:16, cols] = tile - sky[8:16, cols]
            else:
                for n in range(8):
                    out[7 - n : 8 - n, cols] = tile[n : n + 1] - sky[7 - n : 8 - n, cols]


def on_device(grid_cells, visibilities, weights, layer_index, group_index, plane_depths, sky_model):
    vmem = pl.BlockSpec(memory_space=pltpu.VMEM)
    smem = pl.BlockSpec(memory_space=pltpu.SMEM)
    vals, misc = pl.pallas_call(
        functools.partial(exchange_kernel, 1),
        out_shape=(
            jax.ShapeDtypeStruct((4, LAYERS * CAP, LANES), F32),
            jax.ShapeDtypeStruct((2, SOURCES, LANES), F32),
        ),
        in_specs=[vmem] * 5 + [smem],
        out_specs=(vmem, vmem),
        scratch_shapes=[
            pltpu.VMEM((GROUPS, MSG, LANES), F32),
            pltpu.VMEM((SOURCES, MSG, LANES), F32),
            pltpu.SemaphoreType.DMA,
            pltpu.SemaphoreType.DMA,
        ],
        compiler_params=pltpu.CompilerParams(collective_id=0, has_side_effects=True),
        name="exchange",
    )(
        grid_cells,
        visibilities,
        weights.reshape(1, VIS_DEV),
        layer_index.reshape(1, VIS_DEV),
        group_index.reshape(1, VIS_DEV),
        plane_depths,
    )
    first_row = (lax.axis_index("wa") * ROWS).astype(I32).reshape(1)
    sky = sky_model[0]
    residual = pl.pallas_call(
        image_kernel,
        out_shape=jax.ShapeDtypeStruct((ROWS, COLS), F32),
        in_specs=[smem, vmem, vmem, vmem],
        out_specs=vmem,
        scratch_shapes=[
            pltpu.VMEM((LAYERS * 32 * 8, LANES), F32),
            pltpu.VMEM((LAYERS * 16 * 8, LANES), F32),
            pltpu.VMEM((LAYERS * 64 * 8, LANES), F32),
            pltpu.VMEM((LAYERS * 8, LANES), F32),
            pltpu.VMEM((64 * 8, LANES), F32),
            pltpu.VMEM((64 * 8, LANES), F32),
            pltpu.VMEM((512, 256), F32),
            pltpu.VMEM((512, 1024), BF16),
            pltpu.VMEM((256, 1024), BF16),
            pltpu.VMEM((512, 1024), BF16),
            pltpu.VMEM((256, 1024), BF16),
        ],
        compiler_params=pltpu.CompilerParams(vmem_limit_bytes=60 * 1024 * 1024),
        name="image",
    )(first_row, vals, misc, sky)
    return residual[None]


def solution(mesh):
    both = ("wa", "ch")
    return jax.shard_map(
        on_device,
        mesh=mesh,
        in_specs=(
            P(None, both),
            P(None, both),
            P(both),
            P(both),
            P(both),
            P("wa"),
            P("ch", "wa", None),
        ),
        out_specs=P("ch", "wa", None),
        check_vma=False,
    )
```

```python
import functools
import math

import jax
import jax.numpy as jnp
from jax import lax
from jax.experimental import pallas as pl
from jax.experimental.pallas import tpu as pltpu
from jax.sharding import PartitionSpec as P

F32 = jnp.float32
BF16 = jnp.bfloat16
I32 = jnp.int32

GRID = 8192
LAYERS = 32
GROUPS = 4
SOURCES = 128
CAP = 8
LANES = 128
VIS_DEV = 512
ROWS = 16
COLS = 4096
BLOCKS = COLS // 256
MSG = 10

SIN_C = (4.442882919124344, -7.308245686509099, 3.6063542184331383, -0.8461116503741475, 0.10982451642439378)
COS_C = (1.4142134962552289, -6.978850948563853, 5.7394603769076955, -1.8835579059892091, 0.31068802753070307)


def horner(g, coefs):
    total = coefs[-1] * g + coefs[-2]
    for c in coefs[-3::-1]:
        total = total * g + c
    return total


def sincos_turns(f):
    g = f * f
    s = horner(g, SIN_C) * f
    c = horner(g, COS_C)
    return 1.0 - s * s, s * c


def sincos_phase(p):
    q = ((p + GRID) & (2 * GRID - 1)) - GRID
    return sincos_turns(q.astype(F32) * (1.0 / (2 * GRID)))


def cmul(a, b):
    return a[0] * b[0] - a[1] * b[1], a[0] * b[1] + a[1] * b[0]


def fill_blocks(cells, vis, weights, layer, group, depth, out):
    w = weights[...]
    target_row = (layer[...] * GROUPS + group[...]).astype(F32)
    blocks = VIS_DEV // LANES
    lane = lax.broadcasted_iota(I32, (LANES, LANES), 1)
    sub = lax.broadcasted_iota(I32, (LANES, LANES), 0)
    slots = []
    for b in range(blocks):
        mine = target_row[:, b * LANES : (b + 1) * LANES]
        across = jnp.broadcast_to(mine, (LANES, LANES)).T
        hits = jnp.where((across == mine) & (lane < sub), 1.0, 0.0)
        for other in range(b):
            theirs = target_row[:, other * LANES : (other + 1) * LANES]
            hits += jnp.where(across == theirs, 1.0, 0.0)
        rank = jnp.sum(hits, axis=1, keepdims=True).astype(I32)
        t = across.astype(I32)
        slots.append((t & 3) * (LAYERS * CAP) + (t >> 2) * CAP + rank)
    zero = jnp.zeros((1, VIS_DEV), F32)
    values = jnp.concatenate(
        [
            w * vis[0:1, :],
            w * vis[1:2, :],
            cells[0:1, :].astype(F32),
            cells[1:2, :].astype(F32),
            zero,
            zero,
            zero,
            zero,
        ],
        0,
    )
    high = values.astype(BF16)
    rest = values - high.astype(F32)
    middle = rest.astype(BF16)
    low = (rest - middle.astype(F32)).astype(BF16)
    for group_number in range(GROUPS):
        for half in range(2):
            first = (group_number * 2 + half) * LANES
            picks = jnp.concatenate(
                [jnp.where(slots[b] == lane + first, 1.0, 0.0).astype(BF16) for b in range(blocks)], 0
            )
            total = jnp.dot(high, picks, preferred_element_type=F32)
            total += jnp.dot(middle, picks, preferred_element_type=F32)
            total += jnp.dot(low, picks, preferred_element_type=F32)
            out[group_number, half * 4 : half * 4 + 4, :] = total[0:4]
        power = jnp.sum(jnp.where(group[...] == group_number, w * w, 0.0), axis=1, keepdims=True)
        out[group_number, 8:9, :] = jnp.zeros((1, LANES), F32) + depth[0]
        out[group_number, 9:10, :] = jnp.zeros((1, LANES), F32) + power


def exchange_kernel(mult, cells, vis, weights, layer, group, depth, vals, misc, blocks, recv, send_sem, recv_sem):
    wa = lax.axis_index("wa")
    ch = lax.axis_index("ch")
    me = wa * GROUPS + ch
    barrier = pltpu.get_barrier_semaphore()

    def device(d):
        other = lax.rem(me + lax.rem(d * mult, SOURCES), SOURCES)
        return other // GROUPS, lax.rem(other, GROUPS)

    def greet(d, carry):
        pl.semaphore_signal(barrier, inc=1, device_id=device(d), device_id_type=pl.DeviceIdType.MESH)
        return carry

    lax.fori_loop(1, SOURCES, greet, 0)
    fill_blocks(cells, vis, weights, layer, group, depth, blocks)
    pl.semaphore_wait(barrier, SOURCES - 1)

    def send(d, carry):
        to = device(d)
        pltpu.make_async_remote_copy(
            src_ref=blocks.at[to[1]],
            dst_ref=recv.at[me],
            send_sem=send_sem,
            recv_sem=recv_sem,
            device_id=to,
            device_id_type=pl.DeviceIdType.MESH,
        ).start()
        return carry

    lax.fori_loop(1, SOURCES, send, 0)
    recv[me] = blocks[ch]
    rest = recv.at[pl.ds(0, SOURCES - 1)]
    pltpu.make_async_copy(rest, rest, recv_sem).wait()
    for half in range(2):
        for v in range(4):
            vals[v, half * LANES : (half + 1) * LANES, :] = recv[:, half * 4 + v, :].T
    misc[0] = recv[:, 8, :]
    misc[1] = recv[:, 9, :]
    pltpu.make_async_copy(rest, rest, send_sem).wait()


def image_kernel(first_row, vals, misc, sky, out, wtab, ltab, ntab, c16, dterm, acc, ximg):
    row0 = first_row[0]
    sub = lax.broadcasted_iota(I32, (8, LANES), 0)
    lane = lax.broadcasted_iota(I32, (8, LANES), 1)
    for sl in range(2):
        rows = (row0 + 768) + (8 + sub if sl == 0 else 7 - sub)
        l = 0.8 * rows.astype(F32) / GRID
        for sn in range(2):
            for c0 in range(BLOCKS):
                cols = 256 * c0 - 1024 + (128 + lane if sn == 0 else 127 - lane)
                m = 0.8 * cols.astype(F32) / GRID
                q = l * l + m * m
                t = (c0 * 2 + sl) * 2 + sn
                dterm[t * 8 : t * 8 + 8, :] = -q / (1.0 + jnp.sqrt(1.0 - q))
    acc[...] = jnp.zeros_like(acc)

    def tables(jc, carry):
        base = pl.multiple_of(jc * 32, 32)
        zr = vals[0, pl.ds(base, 32), :]
        zi = vals[1, pl.ds(base, 32), :]
        u = vals[2, pl.ds(base, 32), :].astype(I32)
        v = vals[3, pl.ds(base, 32), :].astype(I32)

        def put(ref, per_layer, q, x):
            for i in range(4):
                at = pl.multiple_of((jc * 4 + i) * per_layer * 8, 8) + q * 8
                ref[pl.ds(at, 8), :] = x[i * 8 : i * 8 + 8]

        w = cmul((zr, zi), sincos_phase((2 * row0 + 1551) * u - 1793 * v))
        step = sincos_phase(512 * v)
        for c0 in range(BLOCKS):
            put(wtab, 32, c0 * 2, w[0])
            put(wtab, 32, c0 * 2 + 1, w[1])
            if c0 + 1 < BLOCKS:
                w = cmul(w, step)
        half_step = sincos_phase(u)
        step = cmul(half_step, half_step)
        e = half_step
        for n in range(8):
            put(ltab, 16, n, e[0])
            put(ltab, 16, 8 + n, e[1])
            if n < 7:
                e = cmul(e, step)
        half_step = sincos_phase(v)
        step = cmul(half_step, half_step)
        e = half_step
        for n in range(16):
            put(ntab, 64, n, e[0])
            put(ntab, 64, 15 - n + 16, e[0])
            put(ntab, 64, n + 32, e[1])
            put(ntab, 64, 15 - n + 48, -e[1])
            if n < 15:
                e = cmul(e, step)
        c16[pl.ds(base, 32), :] = 2.0 * sincos_phase(32 * v)[0]
        return carry

    lax.fori_loop(0, LAYERS // 4, tables, 0)

    def expand(j, lhs, rhs):
        for s in range(8):
            ks = slice(s * LANES, (s + 1) * LANES)
            lbase = ltab[pl.ds(j * 128 + s, 16, stride=8), :]
            for q in range(32):
                row = wtab[pl.ds(j * 256 + q * 8 + s, 1), :]
                lhs[q * 16 : q * 16 + 16, ks] = (lbase * row).astype(BF16)
            c2 = c16[pl.ds(j * 8 + s, 1), :]
            for part in range(2):
                now = ntab[pl.ds(j * 512 + part * 256 + s, 16, stride=8), :]
                last = ntab[pl.ds(j * 512 + part * 256 + 128 + s, 16, stride=8), :]
                for b in range(8):
                    rhs[part * 128 + b * 16 : part * 128 + b * 16 + 16, ks] = now.astype(BF16)
                    if b < 7:
                        now, last = c2 * now - last, now

    def image(j, lhs, rhs):
        ximg[...] = lax.dot_general(
            lhs[...], rhs[...], (((1,), (1,)), ((), ())), preferred_element_type=F32
        )
        depth = misc[0, pl.ds(j * GROUPS, 1), :]
        for c0 in range(BLOCKS):
            parts = []
            for ri in range(2):
                at = (c0 * 2 + ri) * 16
                cc = ximg[at : at + 8, 0:LANES]
                cs = ximg[at : at + 8, LANES:]
                sc = ximg[at + 8 : at + 16, 0:LANES]
                ss = ximg[at + 8 : at + 16, LANES:]
                parts.append((cc - ss, cc + ss, sc + cs, sc - cs))
            (ra, rb, rp, rm), (ia, ib, ip, im) = parts
            pixels = ((ra - ip, ia + rp), (rb - im, ib + rm), (rb + im, ib - rm), (ra + ip, ia - rp))
            for k, (pr, pi) in enumerate(pixels):
                at = (c0 * 4 + k) * 8
                t = depth * dterm[at : at + 8, :]
                cos, sin = sincos_turns(t - jnp.round(t))
                acc[at : at + 8, :] += cos * pr - sin * pi

    def all_layers(lhs_a, rhs_a, lhs_b, rhs_b):
        expand(0, lhs_a, rhs_a)

        def pair(jj, carry):
            expand(2 * jj + 1, lhs_b, rhs_b)
            image(2 * jj, lhs_a, rhs_a)
            expand(jnp.minimum(2 * jj + 2, LAYERS - 1), lhs_a, rhs_a)
            image(2 * jj + 1, lhs_b, rhs_b)
            return carry

        lax.fori_loop(0, LAYERS // 2, pair, 0)

    pl.run_scoped(
        all_layers,
        pltpu.VMEM((512, 1024), BF16),
        pltpu.VMEM((256, 1024), BF16),
        pltpu.VMEM((512, 1024), BF16),
        pltpu.VMEM((256, 1024), BF16),
    )

    noise = jnp.sum(misc[1], axis=0, keepdims=True)
    scale = lax.rsqrt(noise)
    back_lane = (LANES - 1) - lane
    for c0 in range(BLOCKS):
        for k in range(4):
            at = (c0 * 4 + k) * 8
            tile = acc[at : at + 8, :] * scale
            if k % 2 == 1:
                tile = jnp.take_along_axis(tile, back_lane, axis=1, mode="promise_in_bounds")
            cols = slice(c0 * 256 + (128 if k % 2 == 0 else 0), c0 * 256 + (256 if k % 2 == 0 else 128))
            if k < 2:
                out[8:16, cols] = tile - sky[8:16, cols]
            else:
                for n in range(8):
                    out[7 - n : 8 - n, cols] = tile[n : n + 1] - sky[7 - n : 8 - n, cols]


def on_device(grid_cells, visibilities, weights, layer_index, group_index, plane_depths, sky_model):
    vmem = pl.BlockSpec(memory_space=pltpu.VMEM)
    smem = pl.BlockSpec(memory_space=pltpu.SMEM)
    vals, misc = pl.pallas_call(
        functools.partial(exchange_kernel, 1),
        out_shape=(
            jax.ShapeDtypeStruct((4, LAYERS * CAP, LANES), F32),
            jax.ShapeDtypeStruct((2, SOURCES, LANES), F32),
        ),
        in_specs=[vmem] * 5 + [smem],
        out_specs=(vmem, vmem),
        scratch_shapes=[
            pltpu.VMEM((GROUPS, MSG, LANES), F32),
            pltpu.VMEM((SOURCES, MSG, LANES), F32),
            pltpu.SemaphoreType.DMA,
            pltpu.SemaphoreType.DMA,
        ],
        compiler_params=pltpu.CompilerParams(collective_id=0, has_side_effects=True),
        name="exchange",
    )(
        grid_cells,
        visibilities,
        weights.reshape(1, VIS_DEV),
        layer_index.reshape(1, VIS_DEV),
        group_index.reshape(1, VIS_DEV),
        plane_depths,
    )
    first_row = (lax.axis_index("wa") * ROWS).astype(I32).reshape(1)
    sky = sky_model[0]
    residual = pl.pallas_call(
        image_kernel,
        out_shape=jax.ShapeDtypeStruct((ROWS, COLS), F32),
        in_specs=[smem, vmem, vmem, vmem],
        out_specs=vmem,
        scratch_shapes=[
            pltpu.VMEM((LAYERS * 32 * 8, LANES), F32),
            pltpu.VMEM((LAYERS * 16 * 8, LANES), F32),
            pltpu.VMEM((LAYERS * 64 * 8, LANES), F32),
            pltpu.VMEM((LAYERS * 8, LANES), F32),
            pltpu.VMEM((64 * 8, LANES), F32),
            pltpu.VMEM((64 * 8, LANES), F32),
            pltpu.VMEM((512, 256), F32),
        ],
        compiler_params=pltpu.CompilerParams(vmem_limit_bytes=60 * 1024 * 1024),
        name="image",
    )(first_row, vals, misc, sky)
    return residual[None]


def solution(mesh):
    both = ("wa", "ch")
    return jax.shard_map(
        on_device,
        mesh=mesh,
        in_specs=(
            P(None, both),
            P(None, both),
            P(both),
            P(both),
            P(both),
            P("wa"),
            P("ch", "wa", None),
        ),
        out_specs=P("ch", "wa", None),
        check_vma=False,
    )
```

```python
import functools
import math

import jax
import jax.numpy as jnp
from jax import lax
from jax.experimental import pallas as pl
from jax.experimental.pallas import tpu as pltpu
from jax.sharding import PartitionSpec as P

F32 = jnp.float32
BF16 = jnp.bfloat16
I32 = jnp.int32

GRID = 8192
LAYERS = 32
GROUPS = 4
SOURCES = 128
CAP = 8
LANES = 128
VIS_DEV = 512
ROWS = 16
COLS = 4096
BLOCKS = COLS // 256
ALL = SOURCES - 1

SIN_C = (4.442882919124344, -7.308245686509099, 3.6063542184331383, -0.8461116503741475, 0.10982451642439378)
COS_C = (1.4142134962552289, -6.978850948563853, 5.7394603769076955, -1.8835579059892091, 0.31068802753070307)


def horner(g, coefs):
    total = coefs[-1] * g + coefs[-2]
    for c in coefs[-3::-1]:
        total = total * g + c
    return total


def sincos_turns(f):
    g = f * f
    s = horner(g, SIN_C) * f
    c = horner(g, COS_C)
    return 1.0 - s * s, s * c


def half_turns(f):
    g = f * f
    return horner(g, SIN_C) * f, horner(g, COS_C)


def csquare(a):
    return a[0] * a[0] - a[1] * a[1], 2.0 * (a[0] * a[1])


def sincos_phase(p):
    q = ((p + GRID) & (2 * GRID - 1)) - GRID
    return sincos_turns(q.astype(F32) * (1.0 / (2 * GRID)))


def cmul(a, b):
    return a[0] * b[0] - a[1] * b[1], a[0] * b[1] + a[1] * b[0]


def fill_blocks(cells, vis, weights, layer, group, depth, blocks, notes):
    w = weights[...]
    target_row = (layer[...] * GROUPS + group[...]).astype(F32)
    pieces = VIS_DEV // LANES
    lane = lax.broadcasted_iota(I32, (LANES, LANES), 1)
    sub = lax.broadcasted_iota(I32, (LANES, LANES), 0)
    slots = []
    for b in range(pieces):
        mine = target_row[:, b * LANES : (b + 1) * LANES]
        across = jnp.broadcast_to(mine, (LANES, LANES)).T
        hits = jnp.where((across == mine) & (lane < sub), 1.0, 0.0)
        for other in range(b):
            theirs = target_row[:, other * LANES : (other + 1) * LANES]
            hits += jnp.where(across == theirs, 1.0, 0.0)
        rank = jnp.sum(hits, axis=1, keepdims=True).astype(I32)
        t = across.astype(I32)
        slots.append((t & 3) * (LAYERS * CAP) + (t >> 2) * CAP + rank)
    zero = jnp.zeros((1, VIS_DEV), F32)
    values = jnp.concatenate(
        [
            w * vis[0:1, :],
            w * vis[1:2, :],
            cells[0:1, :].astype(F32),
            cells[1:2, :].astype(F32),
            zero,
            zero,
            zero,
            zero,
        ],
        0,
    )
    high = values.astype(BF16)
    rest = values - high.astype(F32)
    middle = rest.astype(BF16)
    low = (rest - middle.astype(F32)).astype(BF16)
    for group_number in range(GROUPS):
        for half in range(2):
            first = (group_number * 2 + half) * LANES
            picks = jnp.concatenate(
                [jnp.where(slots[b] == lane + first, 1.0, 0.0).astype(BF16) for b in range(pieces)], 0
            )
            total = jnp.dot(high, picks, preferred_element_type=F32)
            total += jnp.dot(middle, picks, preferred_element_type=F32)
            total += jnp.dot(low, picks, preferred_element_type=F32)
            blocks[group_number, half] = total[0:4]
        power = jnp.sum(jnp.where(group[...] == group_number, w * w, 0.0), axis=1, keepdims=True)
        notes[group_number, 0:1, :] = jnp.zeros((1, LANES), F32) + depth[0]
        notes[group_number, 1:2, :] = jnp.zeros((1, LANES), F32) + power


def kernel(
    cells, vis, weights, layer, group, depth, sky, out,
    blocks, notes, recv, heard, vals, wtab, ltab, ntab, c8, dterm, stab, ctab, acc, x_a, x_b,
    send_sem, recv_sem, note_send, note_recv,
):
    wa = lax.axis_index("wa")
    ch = lax.axis_index("ch")
    me = wa * GROUPS + ch
    row0 = wa * ROWS
    barrier = pltpu.get_barrier_semaphore()
    mesh_id = pl.DeviceIdType.MESH

    def each_peer(act):
        for i in range(1, GROUPS):
            act(wa, lax.rem(ch + i, GROUPS))

        def several(d, carry):
            other = lax.rem(wa + d, LAYERS)
            for c in range(GROUPS):
                act(other, c)
            return carry

        lax.fori_loop(1, LAYERS, several, 0)

    def greet(w, c):
        pl.semaphore_signal(barrier, inc=1, device_id=(w, c), device_id_type=mesh_id)

    each_peer(greet)
    fill_blocks(cells, vis, weights, layer, group, depth, blocks, notes)
    sub = lax.broadcasted_iota(I32, (8, LANES), 0)
    lane = lax.broadcasted_iota(I32, (8, LANES), 1)
    for sl in range(2):
        rows = (row0 + 768) + (8 + sub if sl == 0 else 7 - sub)
        l = 0.8 * rows.astype(F32) / GRID
        for sn in range(2):
            for c0 in range(BLOCKS):
                cols = 256 * c0 - 1024 + (128 + lane if sn == 0 else 127 - lane)
                m = 0.8 * cols.astype(F32) / GRID
                q = l * l + m * m
                t = (c0 * 2 + sl) * 2 + sn
                dterm[t * 8 : t * 8 + 8, :] = -q / (1.0 + jnp.sqrt(1.0 - q))
    acc[...] = jnp.zeros_like(acc)
    pl.semaphore_wait(barrier, ALL)

    def send_note(w, c):
        pltpu.make_async_remote_copy(
            src_ref=notes.at[c], dst_ref=heard.at[me], send_sem=note_send, recv_sem=note_recv,
            device_id=(w, c), device_id_type=mesh_id,
        ).start()

    each_peer(send_note)
    for half in range(2):

        def send(w, c):
            pltpu.make_async_remote_copy(
                src_ref=blocks.at[c, half], dst_ref=recv.at[half, me],
                send_sem=send_sem.at[half], recv_sem=recv_sem.at[half],
                device_id=(w, c), device_id_type=mesh_id,
            ).start()

        each_peer(send)
    for half in range(2):
        recv[half, me] = blocks[ch, half]
    heard[me] = notes[ch]

    all_notes = heard.at[pl.ds(0, ALL)]
    pltpu.make_async_copy(all_notes, all_notes, note_recv).wait()

    def screens(j, carry):
        w = heard[j * GROUPS, 0:1, :]
        for p in range(64):
            t = w * dterm[p * 8 : p * 8 + 8, :]
            s, c = half_turns(t - jnp.round(t))
            stab[j, p * 8 : p * 8 + 8, :] = s
            ctab[j, p * 8 : p * 8 + 8, :] = c
        return carry

    lax.fori_loop(0, LAYERS, screens, 0)

    def tables(jc, carry):
        base = pl.multiple_of(jc * 32, 32)
        zr = vals[0, pl.ds(base, 32), :]
        zi = vals[1, pl.ds(base, 32), :]
        u = vals[2, pl.ds(base, 32), :].astype(I32)
        v = vals[3, pl.ds(base, 32), :].astype(I32)

        def put(ref, per_layer, q, x):
            for i in range(4):
                at = pl.multiple_of((jc * 4 + i) * per_layer * 8, 8) + q * 8
                ref[pl.ds(at, 8), :] = x[i * 8 : i * 8 + 8]

        w = cmul((zr, zi), sincos_phase((2 * row0 + 1551) * u - 1793 * v))
        step = sincos_phase(512 * v)
        for c0 in range(BLOCKS):
            put(wtab, 32, c0 * 2, w[0])
            put(wtab, 32, c0 * 2 + 1, w[1])
            if c0 + 1 < BLOCKS:
                w = cmul(w, step)
        e = sincos_phase(u)
        step = csquare(e)
        for n in range(8):
            put(ltab, 16, n, e[0])
            put(ltab, 16, 8 + n, e[1])
            if n < 7:
                e = cmul(e, step)
        e = sincos_phase(v)
        step = csquare(e)
        eighth = csquare(csquare(csquare(step)))
        for n in range(8):
            put(ntab, 32, n, e[0])
            put(ntab, 32, 15 - n, e[0])
            put(ntab, 32, 16 + n, e[1])
            put(ntab, 32, 31 - n, e[1])
            if n < 7:
                e = cmul(e, step)
        c8[pl.ds(base, 32), :] = 2.0 * eighth[0]
        return carry

    def expand(j, lhs, rhs):
        for s in range(8):
            ks = slice(s * LANES, (s + 1) * LANES)
            lbase = ltab[pl.ds(j * 128 + s, 16, stride=8), :]
            for q in range(32):
                row = wtab[pl.ds(j * 256 + q * 8 + s, 1), :]
                lhs[q * 16 : q * 16 + 16, ks] = (lbase * row).astype(BF16)
            c2 = c8[pl.ds(j * 8 + s, 1), :]
            for part in range(2):
                low = ntab[pl.ds(j * 256 + part * 128 + s, 8, stride=8), :]
                back = ntab[pl.ds(j * 256 + part * 128 + 64 + s, 8, stride=8), :]
                high = c2 * low - back if part == 0 else c2 * low + back
                for b in range(8):
                    at = part * 128 + b * 16
                    rhs[at : at + 16, ks] = jnp.concatenate([low, high], 0).astype(BF16)
                    if b < 7:
                        low = c2 * high - low
                        high = c2 * low - high

    def multiply(ximg, lhs, rhs):
        ximg[...] = lax.dot_general(
            lhs[...], rhs[...], (((1,), (1,)), ((), ())), preferred_element_type=F32
        )

    def image(j, ximg):
        for c0 in range(BLOCKS):
            parts = []
            for ri in range(2):
                at = (c0 * 2 + ri) * 16
                cc = ximg[at : at + 8, 0:LANES]
                cs = ximg[at : at + 8, LANES:]
                sc = ximg[at + 8 : at + 16, 0:LANES]
                ss = ximg[at + 8 : at + 16, LANES:]
                parts.append((cc - ss, cc + ss, sc + cs, sc - cs))
            (ra, rb, rp, rm), (ia, ib, ip, im) = parts
            pixels = ((ra - ip, ia + rp), (rb - im, ib + rm), (rb + im, ib - rm), (ra + ip, ia - rp))
            for k, (pr, pi) in enumerate(pixels):
                at = (c0 * 4 + k) * 8
                s = stab[j, at : at + 8, :]
                c = ctab[j, at : at + 8, :]
                acc[at : at + 8, :] += pr - s * (s * pr + c * pi)

    def all_layers(lhs_a, rhs_a, lhs_b, rhs_b):
        def part(half, carry):
            arriving = recv.at[half, pl.ds(0, ALL)]
            pltpu.make_async_copy(arriving, arriving, recv_sem.at[half]).wait()
            for v in range(4):
                vals[v, pl.ds(pl.multiple_of(half * LANES, LANES), LANES), :] = recv[half, :, v, :].T
            first = half * (LAYERS // 2)
            lax.fori_loop(half * 4, half * 4 + 4, tables, 0)
            expand(first, lhs_a, rhs_a)
            multiply(x_a, lhs_a, rhs_a)
            expand(first + 1, lhs_b, rhs_b)

            def pair(jj, carry):
                j = first + 2 * jj
                last = first + LAYERS // 2 - 1
                multiply(x_b, lhs_b, rhs_b)
                image(j, x_a)
                expand(jnp.minimum(j + 2, last), lhs_a, rhs_a)
                multiply(x_a, lhs_a, rhs_a)
                image(j + 1, x_b)
                expand(jnp.minimum(j + 3, last), lhs_b, rhs_b)
                return carry

            lax.fori_loop(0, LAYERS // 4, pair, 0)
            return carry

        lax.fori_loop(0, 2, part, 0)

    pl.run_scoped(
        all_layers,
        pltpu.VMEM((512, 1024), BF16),
        pltpu.VMEM((256, 1024), BF16),
        pltpu.VMEM((512, 1024), BF16),
        pltpu.VMEM((256, 1024), BF16),
    )

    noise = jnp.sum(heard[:, 1, :], axis=0, keepdims=True)
    scale = lax.rsqrt(noise)
    back_lane = (LANES - 1) - lane
    for c0 in range(BLOCKS):
        for k in range(4):
            at = (c0 * 4 + k) * 8
            tile = acc[at : at + 8, :] * scale
            if k % 2 == 1:
                tile = jnp.take_along_axis(tile, back_lane, axis=1, mode="promise_in_bounds")
            cols = slice(c0 * 256 + (128 if k % 2 == 0 else 0), c0 * 256 + (256 if k % 2 == 0 else 128))
            if k < 2:
                out[8:16, cols] = tile - sky[8:16, cols]
            else:
                for n in range(8):
                    out[7 - n : 8 - n, cols] = tile[n : n + 1] - sky[7 - n : 8 - n, cols]
    pltpu.make_async_copy(all_notes, all_notes, note_send).wait()
    for half in range(2):
        sent = recv.at[half, pl.ds(0, ALL)]
        pltpu.make_async_copy(sent, sent, send_sem.at[half]).wait()


def on_device(grid_cells, visibilities, weights, layer_index, group_index, plane_depths, sky_model):
    vmem = pl.BlockSpec(memory_space=pltpu.VMEM)
    smem = pl.BlockSpec(memory_space=pltpu.SMEM)
    residual = pl.pallas_call(
        kernel,
        out_shape=jax.ShapeDtypeStruct((ROWS, COLS), F32),
        in_specs=[vmem] * 5 + [smem, vmem],
        out_specs=vmem,
        scratch_shapes=[
            pltpu.VMEM((GROUPS, 2, 4, LANES), F32),
            pltpu.VMEM((GROUPS, 2, LANES), F32),
            pltpu.VMEM((2, SOURCES, 4, LANES), F32),
            pltpu.VMEM((SOURCES, 2, LANES), F32),
            pltpu.VMEM((4, LAYERS * CAP, LANES), F32),
            pltpu.VMEM((LAYERS * 32 * 8, LANES), F32),
            pltpu.VMEM((LAYERS * 16 * 8, LANES), F32),
            pltpu.VMEM((LAYERS * 32 * 8, LANES), F32),
            pltpu.VMEM((LAYERS * 8, LANES), F32),
            pltpu.VMEM((64 * 8, LANES), F32),
            pltpu.VMEM((LAYERS, 64 * 8, LANES), F32),
            pltpu.VMEM((LAYERS, 64 * 8, LANES), F32),
            pltpu.VMEM((64 * 8, LANES), F32),
            pltpu.VMEM((512, 256), F32),
            pltpu.VMEM((512, 256), F32),
            pltpu.SemaphoreType.DMA((2,)),
            pltpu.SemaphoreType.DMA((2,)),
            pltpu.SemaphoreType.DMA,
            pltpu.SemaphoreType.DMA,
        ],
        compiler_params=pltpu.CompilerParams(
            collective_id=0, has_side_effects=True, vmem_limit_bytes=60 * 1024 * 1024
        ),
        name="cycle",
    )(
        grid_cells,
        visibilities,
        weights.reshape(1, VIS_DEV),
        layer_index.reshape(1, VIS_DEV),
        group_index.reshape(1, VIS_DEV),
        plane_depths,
        sky_model[0],
    )
    return residual[None]


def solution(mesh):
    both = ("wa", "ch")
    return jax.shard_map(
        on_device,
        mesh=mesh,
        in_specs=(
            P(None, both),
            P(None, both),
            P(both),
            P(both),
            P(both),
            P("wa"),
            P("ch", "wa", None),
        ),
        out_specs=P("ch", "wa", None),
        check_vma=False,
    )
```

```python
import functools
import math

import jax
import jax.numpy as jnp
from jax import lax
from jax.experimental import pallas as pl
from jax.experimental.pallas import tpu as pltpu
from jax.sharding import PartitionSpec as P

F32 = jnp.float32
BF16 = jnp.bfloat16
I32 = jnp.int32

GRID = 8192
LAYERS = 32
GROUPS = 4
SOURCES = 128
CAP = 8
LANES = 128
VIS_DEV = 512
ROWS = 16
COLS = 4096
BLOCKS = COLS // 256
ALL = SOURCES - 1
STAGES = ((0, 0), (0, 1), (1, 0), (3, 0), (1, 1), (3, 1), (2, 0), (2, 1))

SIN_C = (4.442882919124344, -7.308245686509099, 3.6063542184331383, -0.8461116503741475, 0.10982451642439378)
COS_C = (1.4142134962552289, -6.978850948563853, 5.7394603769076955, -1.8835579059892091, 0.31068802753070307)


def horner(g, coefs):
    total = coefs[-1] * g + coefs[-2]
    for c in coefs[-3::-1]:
        total = total * g + c
    return total


def sincos_turns(f):
    g = f * f
    s = horner(g, SIN_C) * f
    c = horner(g, COS_C)
    return 1.0 - s * s, s * c


def half_turns(f):
    g = f * f
    return horner(g, SIN_C) * f, horner(g, COS_C)


def csquare(a):
    return a[0] * a[0] - a[1] * a[1], 2.0 * (a[0] * a[1])


def sincos_phase(p):
    q = ((p + GRID) & (2 * GRID - 1)) - GRID
    return sincos_turns(q.astype(F32) * (1.0 / (2 * GRID)))


def cmul(a, b):
    return a[0] * b[0] - a[1] * b[1], a[0] * b[1] + a[1] * b[0]


def fill_blocks(cells, vis, weights, layer, group, blocks, notes):
    w = weights[...]
    target_row = (layer[...] * GROUPS + group[...]).astype(F32)
    pieces = VIS_DEV // LANES
    lane = lax.broadcasted_iota(I32, (LANES, LANES), 1)
    sub = lax.broadcasted_iota(I32, (LANES, LANES), 0)
    slots = []
    for b in range(pieces):
        mine = target_row[:, b * LANES : (b + 1) * LANES]
        across = jnp.broadcast_to(mine, (LANES, LANES)).T
        hits = jnp.where((across == mine) & (lane < sub), 1.0, 0.0)
        for other in range(b):
            theirs = target_row[:, other * LANES : (other + 1) * LANES]
            hits += jnp.where(across == theirs, 1.0, 0.0)
        rank = jnp.sum(hits, axis=1, keepdims=True).astype(I32)
        t = across.astype(I32)
        slots.append((t & 3) * (LAYERS * CAP) + (t >> 2) * CAP + rank)
    zero = jnp.zeros((1, VIS_DEV), F32)
    values = jnp.concatenate(
        [
            w * vis[0:1, :],
            w * vis[1:2, :],
            cells[0:1, :].astype(F32),
            cells[1:2, :].astype(F32),
            zero,
            zero,
            zero,
            zero,
        ],
        0,
    )
    high = values.astype(BF16)
    rest = values - high.astype(F32)
    middle = rest.astype(BF16)
    low = (rest - middle.astype(F32)).astype(BF16)
    for group_number in range(GROUPS):
        for half in range(2):
            first = (group_number * 2 + half) * LANES
            picks = jnp.concatenate(
                [jnp.where(slots[b] == lane + first, 1.0, 0.0).astype(BF16) for b in range(pieces)], 0
            )
            total = jnp.dot(high, picks, preferred_element_type=F32)
            total += jnp.dot(middle, picks, preferred_element_type=F32)
            total += jnp.dot(low, picks, preferred_element_type=F32)
            blocks[group_number, half] = total[0:4]
        power = jnp.sum(jnp.where(group[...] == group_number, w * w, 0.0), axis=1, keepdims=True)
        notes[group_number] = jnp.zeros((1, LANES), F32) + power


def kernel(
    cells, vis, weights, layer, group, depth, sky, out,
    blocks, notes, recv, heard, mydepth, depths, vals, wtab, ltab, ntab, c8, dterm, stab, ctab, acc, x_a, x_b,
    send_sem, recv_sem, note_send, note_recv, depth_send, depth_recv,
):
    wa = lax.axis_index("wa")
    ch = lax.axis_index("ch")
    me = wa * GROUPS + ch
    row0 = wa * ROWS
    barrier = pltpu.get_barrier_semaphore()
    mesh_id = pl.DeviceIdType.MESH

    def each_peer(act):
        for i in range(1, GROUPS):
            act(wa, lax.rem(ch + i, GROUPS))

        def several(d, carry):
            other = lax.rem(wa + d, LAYERS)
            for c in range(GROUPS):
                act(other, c)
            return carry

        lax.fori_loop(1, LAYERS, several, 0)

    def greet(w, c):
        pl.semaphore_signal(barrier, inc=1, device_id=(w, c), device_id_type=mesh_id)

    each_peer(greet)
    mydepth[0] = jnp.zeros((1, LANES), F32) + depth[0]
    fill_blocks(cells, vis, weights, layer, group, blocks, notes)
    sub = lax.broadcasted_iota(I32, (8, LANES), 0)
    lane = lax.broadcasted_iota(I32, (8, LANES), 1)
    for sl in range(2):
        rows = (row0 + 768) + (8 + sub if sl == 0 else 7 - sub)
        l = 0.8 * rows.astype(F32) / GRID
        for sn in range(2):
            for c0 in range(BLOCKS):
                cols = 256 * c0 - 1024 + (128 + lane if sn == 0 else 127 - lane)
                m = 0.8 * cols.astype(F32) / GRID
                q = l * l + m * m
                t = (c0 * 2 + sl) * 2 + sn
                dterm[t * 8 : t * 8 + 8, :] = -q / (1.0 + jnp.sqrt(1.0 - q))
    acc[...] = jnp.zeros_like(acc)
    pl.semaphore_wait(barrier, ALL)

    x, zy = wa // 8, lax.rem(wa, 8)
    z, y = zy // 4, lax.rem(zy, 4)
    for i, (dx, dz) in enumerate(STAGES):
        for dy in range(4):
            if dx or dz or dy:
                to = lax.rem(x + dx, 4) * 8 + lax.rem(z + dz, 2) * 4 + lax.rem(y + dy, 4)
                pltpu.make_async_remote_copy(
                    src_ref=mydepth.at[0], dst_ref=depths.at[wa],
                    send_sem=depth_send, recv_sem=depth_recv.at[i],
                    device_id=(to, lax.rem(ch + 2 * dz, GROUPS)), device_id_type=mesh_id,
                ).start()
    for half in range(2):

        def send(w, c):
            pltpu.make_async_remote_copy(
                src_ref=blocks.at[c, half], dst_ref=recv.at[half, me],
                send_sem=send_sem.at[half], recv_sem=recv_sem.at[half],
                device_id=(w, c), device_id_type=mesh_id,
            ).start()

        each_peer(send)

    def send_note(w, c):
        pltpu.make_async_remote_copy(
            src_ref=notes.at[c], dst_ref=heard.at[me], send_sem=note_send, recv_sem=note_recv,
            device_id=(w, c), device_id_type=mesh_id,
        ).start()

    each_peer(send_note)
    for half in range(2):
        recv[half, me] = blocks[ch, half]
    heard[me] = notes[ch]
    depths[wa] = mydepth[0]

    for i, (dx, dz) in enumerate(STAGES):
        some = depths.at[pl.ds(0, 4 if i else 3)]
        pltpu.make_async_copy(some, some, depth_recv.at[i]).wait()
        first = lax.rem(x + (4 - dx), 4) * 8 + lax.rem(z + dz, 2) * 4

        def screens(n, carry):
            j = first + n
            w = depths[j]
            for p in range(64):
                t = w * dterm[p * 8 : p * 8 + 8, :]
                s, c = half_turns(t - jnp.round(t))
                stab[j, p * 8 : p * 8 + 8, :] = s
                ctab[j, p * 8 : p * 8 + 8, :] = c
            return carry

        lax.fori_loop(0, 4, screens, 0)

    def tables(jc, carry):
        base = pl.multiple_of(jc * 32, 32)
        zr = vals[0, pl.ds(base, 32), :]
        zi = vals[1, pl.ds(base, 32), :]
        u = vals[2, pl.ds(base, 32), :].astype(I32)
        v = vals[3, pl.ds(base, 32), :].astype(I32)

        def put(ref, per_layer, q, x):
            for i in range(4):
                at = pl.multiple_of((jc * 4 + i) * per_layer * 8, 8) + q * 8
                ref[pl.ds(at, 8), :] = x[i * 8 : i * 8 + 8]

        w = cmul((zr, zi), sincos_phase((2 * row0 + 1551) * u - 1793 * v))
        step = sincos_phase(512 * v)
        for c0 in range(BLOCKS):
            put(wtab, 32, c0 * 2, w[0])
            put(wtab, 32, c0 * 2 + 1, w[1])
            if c0 + 1 < BLOCKS:
                w = cmul(w, step)
        e = sincos_phase(u)
        step = csquare(e)
        for n in range(8):
            put(ltab, 16, n, e[0])
            put(ltab, 16, 8 + n, e[1])
            if n < 7:
                e = cmul(e, step)
        e = sincos_phase(v)
        step = csquare(e)
        eighth = csquare(csquare(csquare(step)))
        for n in range(8):
            put(ntab, 32, n, e[0])
            put(ntab, 32, 15 - n, e[0])
            put(ntab, 32, 16 + n, e[1])
            put(ntab, 32, 31 - n, e[1])
            if n < 7:
                e = cmul(e, step)
        c8[pl.ds(base, 32), :] = 2.0 * eighth[0]
        return carry

    def expand(j, lhs, rhs):
        for s in range(8):
            ks = slice(s * LANES, (s + 1) * LANES)
            lbase = ltab[pl.ds(j * 128 + s, 16, stride=8), :]
            for q in range(32):
                row = wtab[pl.ds(j * 256 + q * 8 + s, 1), :]
                lhs[q * 16 : q * 16 + 16, ks] = (lbase * row).astype(BF16)
            c2 = c8[pl.ds(j * 8 + s, 1), :]
            for part in range(2):
                low = ntab[pl.ds(j * 256 + part * 128 + s, 8, stride=8), :]
                back = ntab[pl.ds(j * 256 + part * 128 + 64 + s, 8, stride=8), :]
                high = c2 * low - back if part == 0 else c2 * low + back
                for b in range(8):
                    at = part * 128 + b * 16
                    rhs[at : at + 16, ks] = jnp.concatenate([low, high], 0).astype(BF16)
                    if b < 7:
                        low = c2 * high - low
                        high = c2 * low - high

    def multiply(ximg, lhs, rhs):
        ximg[...] = lax.dot_general(
            lhs[...], rhs[...], (((1,), (1,)), ((), ())), preferred_element_type=F32
        )

    def image(j, ximg):
        for c0 in range(BLOCKS):
            parts = []
            for ri in range(2):
                at = (c0 * 2 + ri) * 16
                cc = ximg[at : at + 8, 0:LANES]
                cs = ximg[at : at + 8, LANES:]
                sc = ximg[at + 8 : at + 16, 0:LANES]
                ss = ximg[at + 8 : at + 16, LANES:]
                parts.append((cc - ss, cc + ss, sc + cs, sc - cs))
            (ra, rb, rp, rm), (ia, ib, ip, im) = parts
            pixels = ((ra - ip, ia + rp), (rb - im, ib + rm), (rb + im, ib - rm), (ra + ip, ia - rp))
            for k, (pr, pi) in enumerate(pixels):
                at = (c0 * 4 + k) * 8
                s = stab[j, at : at + 8, :]
                c = ctab[j, at : at + 8, :]
                acc[at : at + 8, :] += pr - s * (s * pr + c * pi)

    def arrive(half):
        arriving = recv.at[half, pl.ds(0, ALL)]
        pltpu.make_async_copy(arriving, arriving, recv_sem.at[half]).wait()
        for v in range(4):
            vals[v, half * LANES : (half + 1) * LANES, :] = recv[half, :, v, :].T

    def all_layers(lhs_a, rhs_a, lhs_b, rhs_b):
        arrive(0)
        tables(0, 0)
        expand(0, lhs_a, rhs_a)
        multiply(x_a, lhs_a, rhs_a)
        expand(1, lhs_b, rhs_b)

        def several(jj, carry):
            tables(jnp.minimum(jj + 1, LAYERS // 4 - 1), 0)
            for i in range(0, 4, 2):
                j = 4 * jj + i
                multiply(x_b, lhs_b, rhs_b)
                image(j, x_a)
                expand(jnp.minimum(j + 2, LAYERS - 1), lhs_a, rhs_a)
                multiply(x_a, lhs_a, rhs_a)
                image(j + 1, x_b)
                expand(jnp.minimum(j + 3, LAYERS - 1), lhs_b, rhs_b)
            return carry

        lax.fori_loop(0, LAYERS // 8 - 1, several, 0)
        arrive(1)
        lax.fori_loop(LAYERS // 8 - 1, LAYERS // 4, several, 0)

    pl.run_scoped(
        all_layers,
        pltpu.VMEM((512, 1024), BF16),
        pltpu.VMEM((256, 1024), BF16),
        pltpu.VMEM((512, 1024), BF16),
        pltpu.VMEM((256, 1024), BF16),
    )

    all_notes = heard.at[pl.ds(0, ALL)]
    pltpu.make_async_copy(all_notes, all_notes, note_recv).wait()
    noise = jnp.sum(heard[...], axis=0)
    scale = lax.rsqrt(noise)
    back_lane = (LANES - 1) - lane
    for c0 in range(BLOCKS):
        for k in range(4):
            at = (c0 * 4 + k) * 8
            tile = acc[at : at + 8, :] * scale
            if k % 2 == 1:
                tile = jnp.take_along_axis(tile, back_lane, axis=1, mode="promise_in_bounds")
            cols = slice(c0 * 256 + (128 if k % 2 == 0 else 0), c0 * 256 + (256 if k % 2 == 0 else 128))
            if k < 2:
                out[8:16, cols] = tile - sky[8:16, cols]
            else:
                for n in range(8):
                    out[7 - n : 8 - n, cols] = tile[n : n + 1] - sky[7 - n : 8 - n, cols]
    pltpu.make_async_copy(all_notes, all_notes, note_send).wait()
    others = depths.at[pl.ds(0, LAYERS - 1)]
    pltpu.make_async_copy(others, others, depth_send).wait()
    for half in range(2):
        sent = recv.at[half, pl.ds(0, ALL)]
        pltpu.make_async_copy(sent, sent, send_sem.at[half]).wait()


def on_device(grid_cells, visibilities, weights, layer_index, group_index, plane_depths, sky_model):
    vmem = pl.BlockSpec(memory_space=pltpu.VMEM)
    smem = pl.BlockSpec(memory_space=pltpu.SMEM)
    residual = pl.pallas_call(
        kernel,
        out_shape=jax.ShapeDtypeStruct((ROWS, COLS), F32),
        in_specs=[vmem] * 5 + [smem, vmem],
        out_specs=vmem,
        scratch_shapes=[
            pltpu.VMEM((GROUPS, 2, 4, LANES), F32),
            pltpu.VMEM((GROUPS, 1, LANES), F32),
            pltpu.VMEM((2, SOURCES, 4, LANES), F32),
            pltpu.VMEM((SOURCES, 1, LANES), F32),
            pltpu.VMEM((1, 1, LANES), F32),
            pltpu.VMEM((LAYERS, 1, LANES), F32),
            pltpu.VMEM((4, LAYERS * CAP, LANES), F32),
            pltpu.VMEM((LAYERS * 32 * 8, LANES), F32),
            pltpu.VMEM((LAYERS * 16 * 8, LANES), F32),
            pltpu.VMEM((LAYERS * 32 * 8, LANES), F32),
            pltpu.VMEM((LAYERS * 8, LANES), F32),
            pltpu.VMEM((64 * 8, LANES), F32),
            pltpu.VMEM((LAYERS, 64 * 8, LANES), F32),
            pltpu.VMEM((LAYERS, 64 * 8, LANES), F32),
            pltpu.VMEM((64 * 8, LANES), F32),
            pltpu.VMEM((512, 256), F32),
            pltpu.VMEM((512, 256), F32),
            pltpu.SemaphoreType.DMA((2,)),
            pltpu.SemaphoreType.DMA((2,)),
            pltpu.SemaphoreType.DMA,
            pltpu.SemaphoreType.DMA,
            pltpu.SemaphoreType.DMA,
            pltpu.SemaphoreType.DMA((len(STAGES),)),
        ],
        compiler_params=pltpu.CompilerParams(
            collective_id=0, has_side_effects=True, vmem_limit_bytes=60 * 1024 * 1024
        ),
        name="cycle",
    )(
        grid_cells,
        visibilities,
        weights.reshape(1, VIS_DEV),
        layer_index.reshape(1, VIS_DEV),
        group_index.reshape(1, VIS_DEV),
        plane_depths,
        sky_model[0],
    )
    return residual[None]


def solution(mesh):
    both = ("wa", "ch")
    return jax.shard_map(
        on_device,
        mesh=mesh,
        in_specs=(
            P(None, both),
            P(None, both),
            P(both),
            P(both),
            P(both),
            P("wa"),
            P("ch", "wa", None),
        ),
        out_specs=P("ch", "wa", None),
        check_vma=False,
    )
```

```python
import functools
import math

import jax
import jax.numpy as jnp
from jax import lax
from jax.experimental import pallas as pl
from jax.experimental.pallas import tpu as pltpu
from jax.sharding import PartitionSpec as P

F32 = jnp.float32
BF16 = jnp.bfloat16
I32 = jnp.int32

GRID = 8192
LAYERS = 32
GROUPS = 4
SOURCES = 128
CAP = 8
LANES = 128
VIS_DEV = 512
ROWS = 16
COLS = 4096
BLOCKS = COLS // 256
ALL = SOURCES - 1
FAR_FIRST = (2, 1, 3, 0)
STAGES = ((0, 0), (0, 1), (1, 0), (3, 0), (1, 1), (3, 1), (2, 0), (2, 1))

SIN_C = (4.442882919124344, -7.308245686509099, 3.6063542184331383, -0.8461116503741475, 0.10982451642439378)
COS_C = (1.4142134962552289, -6.978850948563853, 5.7394603769076955, -1.8835579059892091, 0.31068802753070307)


def horner(g, coefs):
    total = coefs[-1] * g + coefs[-2]
    for c in coefs[-3::-1]:
        total = total * g + c
    return total


def sincos_turns(f):
    g = f * f
    s = horner(g, SIN_C) * f
    c = horner(g, COS_C)
    return 1.0 - s * s, s * c


def half_turns(f):
    g = f * f
    return horner(g, SIN_C) * f, horner(g, COS_C)


def csquare(a):
    return a[0] * a[0] - a[1] * a[1], 2.0 * (a[0] * a[1])


def sincos_phase(p):
    q = ((p + GRID) & (2 * GRID - 1)) - GRID
    return sincos_turns(q.astype(F32) * (1.0 / (2 * GRID)))


def cmul(a, b):
    return a[0] * b[0] - a[1] * b[1], a[0] * b[1] + a[1] * b[0]


def fill_blocks(cells, vis, weights, layer, group, blocks, notes):
    w = weights[...]
    target_row = (layer[...] * GROUPS + group[...]).astype(F32)
    pieces = VIS_DEV // LANES
    lane = lax.broadcasted_iota(I32, (LANES, LANES), 1)
    sub = lax.broadcasted_iota(I32, (LANES, LANES), 0)
    slots = []
    for b in range(pieces):
        mine = target_row[:, b * LANES : (b + 1) * LANES]
        across = jnp.broadcast_to(mine, (LANES, LANES)).T
        hits = jnp.where((across == mine) & (lane < sub), 1.0, 0.0)
        for other in range(b):
            theirs = target_row[:, other * LANES : (other + 1) * LANES]
            hits += jnp.where(across == theirs, 1.0, 0.0)
        rank = jnp.sum(hits, axis=1, keepdims=True).astype(I32)
        t = across.astype(I32)
        slots.append((t & 3) * (LAYERS * CAP) + (t >> 2) * CAP + rank)
    zero = jnp.zeros((1, VIS_DEV), F32)
    values = jnp.concatenate(
        [
            w * vis[0:1, :],
            w * vis[1:2, :],
            cells[0:1, :].astype(F32),
            cells[1:2, :].astype(F32),
            zero,
            zero,
            zero,
            zero,
        ],
        0,
    )
    high = values.astype(BF16)
    rest = values - high.astype(F32)
    middle = rest.astype(BF16)
    low = (rest - middle.astype(F32)).astype(BF16)
    for group_number in range(GROUPS):
        for half in range(2):
            first = (group_number * 2 + half) * LANES
            picks = jnp.concatenate(
                [jnp.where(slots[b] == lane + first, 1.0, 0.0).astype(BF16) for b in range(pieces)], 0
            )
            total = jnp.dot(high, picks, preferred_element_type=F32)
            total += jnp.dot(middle, picks, preferred_element_type=F32)
            total += jnp.dot(low, picks, preferred_element_type=F32)
            blocks[group_number, half] = total[0:4]
        power = jnp.sum(jnp.where(group[...] == group_number, w * w, 0.0), axis=1, keepdims=True)
        notes[group_number] = jnp.zeros((1, LANES), F32) + power


def kernel(
    cells_hbm, vis_hbm, weights_hbm, layer_hbm, group_hbm, depth_hbm, out,
    cells, vis, weights, layer, group, depth, load_sem,
    blocks, notes, recv, heard, mydepth, depths, vals, wtab, ltab, ntab, c8, dterm, stab, ctab, acc, x_a, x_b,
    send_sem, recv_sem, note_send, note_recv, depth_send, depth_recv,
):
    wa = lax.axis_index("wa")
    ch = lax.axis_index("ch")
    me = wa * GROUPS + ch
    row0 = wa * ROWS
    loads = [
        pltpu.make_async_copy(src, dst, load_sem.at[i])
        for i, (src, dst) in enumerate(
            (
                (cells_hbm, cells),
                (vis_hbm, vis),
                (weights_hbm, weights),
                (layer_hbm, layer),
                (group_hbm, group),
                (depth_hbm, depth),
            )
        )
    ]
    for load in loads:
        load.start()
    barrier = pltpu.get_barrier_semaphore()
    mesh_id = pl.DeviceIdType.MESH

    x, zy = wa // 8, lax.rem(wa, 8)
    z, y = zy // 4, lax.rem(zy, 4)

    def moved(dx, dz, dy):
        return lax.rem(x + dx, 4) * 8 + lax.rem(z + dz, 2) * 4 + lax.rem(y + dy, 4)

    def each_peer(act):
        for dx in FAR_FIRST:
            for dz in (1, 0):
                for dy in FAR_FIRST:
                    if dx or dz or dy:
                        to = moved(dx, dz, dy)
                        for c in range(GROUPS):
                            act(to, c)
        for i in range(1, GROUPS):
            act(wa, lax.rem(ch + i, GROUPS))

    def greet(w, c):
        pl.semaphore_signal(barrier, inc=1, device_id=(w, c), device_id_type=mesh_id)

    each_peer(greet)
    for load in loads:
        load.wait()
    mydepth[0] = jnp.zeros((1, LANES), F32) + depth[0]
    fill_blocks(cells, vis, weights, layer, group, blocks, notes)
    sub = lax.broadcasted_iota(I32, (8, LANES), 0)
    lane = lax.broadcasted_iota(I32, (8, LANES), 1)
    for sl in range(2):
        rows = (row0 + 768) + (8 + sub if sl == 0 else 7 - sub)
        l = 0.8 * rows.astype(F32) / GRID
        for sn in range(2):
            for c0 in range(BLOCKS):
                cols = 256 * c0 - 1024 + (128 + lane if sn == 0 else 127 - lane)
                m = 0.8 * cols.astype(F32) / GRID
                q = l * l + m * m
                t = (c0 * 2 + sl) * 2 + sn
                dterm[t * 8 : t * 8 + 8, :] = -q / (1.0 + jnp.sqrt(1.0 - q))
    acc[...] = jnp.zeros_like(acc)
    pl.semaphore_wait(barrier, ALL)

    for i, (dx, dz) in enumerate(STAGES):
        for dy in range(4):
            if dx or dz or dy:
                to = moved(dx, dz, dy)
                pltpu.make_async_remote_copy(
                    src_ref=mydepth.at[0], dst_ref=depths.at[wa],
                    send_sem=depth_send, recv_sem=depth_recv.at[i],
                    device_id=(to, lax.rem(ch + 2 * dz, GROUPS)), device_id_type=mesh_id,
                ).start()
    for half in range(2):

        def send(w, c):
            pltpu.make_async_remote_copy(
                src_ref=blocks.at[c, half], dst_ref=recv.at[half, me],
                send_sem=send_sem.at[half], recv_sem=recv_sem.at[half],
                device_id=(w, c), device_id_type=mesh_id,
            ).start()

        each_peer(send)

    def send_note(w, c):
        pltpu.make_async_remote_copy(
            src_ref=notes.at[c], dst_ref=heard.at[me], send_sem=note_send, recv_sem=note_recv,
            device_id=(w, c), device_id_type=mesh_id,
        ).start()

    each_peer(send_note)
    for half in range(2):
        recv[half, me] = blocks[ch, half]
    heard[me] = notes[ch]
    depths[wa] = mydepth[0]

    for i, (dx, dz) in enumerate(STAGES):
        some = depths.at[pl.ds(0, 4 if i else 3)]
        pltpu.make_async_copy(some, some, depth_recv.at[i]).wait()
        first = lax.rem(x + (4 - dx), 4) * 8 + lax.rem(z + dz, 2) * 4

        def screens(n, carry):
            j = first + n
            w = depths[j]
            for p in range(64):
                t = w * dterm[p * 8 : p * 8 + 8, :]
                s, c = half_turns(t - jnp.round(t))
                stab[j, p * 8 : p * 8 + 8, :] = s
                ctab[j, p * 8 : p * 8 + 8, :] = c
            return carry

        lax.fori_loop(0, 4, screens, 0)

    def tables(jc, carry):
        base = pl.multiple_of(jc * 32, 32)
        zr = vals[0, pl.ds(base, 32), :]
        zi = vals[1, pl.ds(base, 32), :]
        u = vals[2, pl.ds(base, 32), :].astype(I32)
        v = vals[3, pl.ds(base, 32), :].astype(I32)

        def put(ref, per_layer, q, x):
            for i in range(4):
                at = pl.multiple_of((jc * 4 + i) * per_layer * 8, 8) + q * 8
                ref[pl.ds(at, 8), :] = x[i * 8 : i * 8 + 8]

        w = cmul((zr, zi), sincos_phase((2 * row0 + 1551) * u - 1793 * v))
        step = sincos_phase(512 * v)
        last, w = w, cmul(w, step)
        put(wtab, 32, 0, last[0])
        put(wtab, 32, 1, last[1])
        twice = step[0] + step[0]
        for c0 in range(1, BLOCKS):
            put(wtab, 32, c0 * 2, w[0])
            put(wtab, 32, c0 * 2 + 1, w[1])
            if c0 + 1 < BLOCKS:
                last, w = w, (twice * w[0] - last[0], twice * w[1] - last[1])
        e = sincos_phase(u)
        last = e[0], -e[1]
        twice = 2.0 - 4.0 * (e[1] * e[1])
        for n in range(8):
            put(ltab, 16, n, e[0])
            put(ltab, 16, 8 + n, e[1])
            if n < 7:
                last, e = e, (twice * e[0] - last[0], twice * e[1] - last[1])
        e = sincos_phase(v)
        step = csquare(e)
        last = e[0], -e[1]
        twice = step[0] + step[0]
        eighth = csquare(csquare(csquare(step)))
        for n in range(8):
            put(ntab, 32, n, e[0])
            put(ntab, 32, 15 - n, e[0])
            put(ntab, 32, 16 + n, e[1])
            put(ntab, 32, 31 - n, e[1])
            if n < 7:
                last, e = e, (twice * e[0] - last[0], twice * e[1] - last[1])
        c8[pl.ds(base, 32), :] = 2.0 * eighth[0]
        return carry

    def expand(j, lhs, rhs):
        for s in range(8):
            ks = slice(s * LANES, (s + 1) * LANES)
            lbase = ltab[pl.ds(j * 128 + s, 16, stride=8), :]
            for q in range(32):
                row = wtab[pl.ds(j * 256 + q * 8 + s, 1), :]
                lhs[q * 16 : q * 16 + 16, ks] = (lbase * row).astype(BF16)
            c2 = c8[pl.ds(j * 8 + s, 1), :]
            for part in range(2):
                low = ntab[pl.ds(j * 256 + part * 128 + s, 8, stride=8), :]
                back = ntab[pl.ds(j * 256 + part * 128 + 64 + s, 8, stride=8), :]
                high = c2 * low - back if part == 0 else c2 * low + back
                for b in range(8):
                    at = part * 128 + b * 16
                    rhs[at : at + 16, ks] = jnp.concatenate([low, high], 0).astype(BF16)
                    if b < 7:
                        low = c2 * high - low
                        high = c2 * low - high

    def multiply(ximg, lhs, rhs):
        ximg[...] = lax.dot_general(
            lhs[...], rhs[...], (((1,), (1,)), ((), ())), preferred_element_type=F32
        )

    def image(j, ximg):
        for c0 in range(BLOCKS):
            parts = []
            for ri in range(2):
                at = (c0 * 2 + ri) * 16
                cc = ximg[at : at + 8, 0:LANES]
                cs = ximg[at : at + 8, LANES:]
                sc = ximg[at + 8 : at + 16, 0:LANES]
                ss = ximg[at + 8 : at + 16, LANES:]
                parts.append((cc - ss, cc + ss, sc + cs, sc - cs))
            (ra, rb, rp, rm), (ia, ib, ip, im) = parts
            pixels = ((ra - ip, ia + rp), (rb - im, ib + rm), (rb + im, ib - rm), (ra + ip, ia - rp))
            for k, (pr, pi) in enumerate(pixels):
                at = (c0 * 4 + k) * 8
                s = stab[j, at : at + 8, :]
                c = ctab[j, at : at + 8, :]
                acc[at : at + 8, :] += pr - s * (s * pr + c * pi)

    def arrive(half):
        arriving = recv.at[half, pl.ds(0, ALL)]
        pltpu.make_async_copy(arriving, arriving, recv_sem.at[half]).wait()
        for v in range(4):
            vals[v, half * LANES : (half + 1) * LANES, :] = recv[half, :, v, :].T

    def all_layers(lhs_a, rhs_a, lhs_b, rhs_b):
        arrive(0)
        tables(0, 0)
        expand(0, lhs_a, rhs_a)
        multiply(x_a, lhs_a, rhs_a)
        expand(1, lhs_b, rhs_b)

        def several(jj, carry):
            tables(jnp.minimum(jj + 1, LAYERS // 4 - 1), 0)
            for i in range(0, 4, 2):
                j = 4 * jj + i
                multiply(x_b, lhs_b, rhs_b)
                image(j, x_a)
                expand(jnp.minimum(j + 2, LAYERS - 1), lhs_a, rhs_a)
                multiply(x_a, lhs_a, rhs_a)
                image(j + 1, x_b)
                expand(jnp.minimum(j + 3, LAYERS - 1), lhs_b, rhs_b)
            return carry

        lax.fori_loop(0, LAYERS // 8 - 1, several, 0)
        arrive(1)
        lax.fori_loop(LAYERS // 8 - 1, LAYERS // 4, several, 0)

    pl.run_scoped(
        all_layers,
        pltpu.VMEM((512, 1024), BF16),
        pltpu.VMEM((256, 1024), BF16),
        pltpu.VMEM((512, 1024), BF16),
        pltpu.VMEM((256, 1024), BF16),
    )

    all_notes = heard.at[pl.ds(0, ALL)]
    pltpu.make_async_copy(all_notes, all_notes, note_recv).wait()
    noise = jnp.sum(heard[...], axis=0)
    scale = lax.rsqrt(noise)
    back_lane = (LANES - 1) - lane
    for c0 in range(BLOCKS):
        for k in range(4):
            at = (c0 * 4 + k) * 8
            tile = acc[at : at + 8, :] * scale
            if k % 2 == 1:
                tile = jnp.take_along_axis(tile, back_lane, axis=1, mode="promise_in_bounds")
            cols = slice(c0 * 256 + (128 if k % 2 == 0 else 0), c0 * 256 + (256 if k % 2 == 0 else 128))
            if k < 2:
                out[8:16, cols] = tile
            else:
                for n in range(8):
                    out[7 - n : 8 - n, cols] = tile[n : n + 1]
    pltpu.make_async_copy(all_notes, all_notes, note_send).wait()
    others = depths.at[pl.ds(0, LAYERS - 1)]
    pltpu.make_async_copy(others, others, depth_send).wait()
    for half in range(2):
        sent = recv.at[half, pl.ds(0, ALL)]
        pltpu.make_async_copy(sent, sent, send_sem.at[half]).wait()


def on_device(grid_cells, visibilities, weights, layer_index, group_index, plane_depths, sky_model):
    vmem = pl.BlockSpec(memory_space=pltpu.VMEM)
    hbm = pl.BlockSpec(memory_space=pltpu.HBM)
    dirty = pl.pallas_call(
        kernel,
        out_shape=jax.ShapeDtypeStruct((ROWS, COLS), F32),
        in_specs=[hbm] * 6,
        out_specs=vmem,
        scratch_shapes=[
            pltpu.VMEM((2, VIS_DEV), I32),
            pltpu.VMEM((2, VIS_DEV), F32),
            pltpu.VMEM((1, VIS_DEV), F32),
            pltpu.VMEM((1, VIS_DEV), I32),
            pltpu.VMEM((1, VIS_DEV), I32),
            pltpu.SMEM((1,), F32),
            pltpu.SemaphoreType.DMA((6,)),
            pltpu.VMEM((GROUPS, 2, 4, LANES), F32),
            pltpu.VMEM((GROUPS, 1, LANES), F32),
            pltpu.VMEM((2, SOURCES, 4, LANES), F32),
            pltpu.VMEM((SOURCES, 1, LANES), F32),
            pltpu.VMEM((1, 1, LANES), F32),
            pltpu.VMEM((LAYERS, 1, LANES), F32),
            pltpu.VMEM((4, LAYERS * CAP, LANES), F32),
            pltpu.VMEM((LAYERS * 32 * 8, LANES), F32),
            pltpu.VMEM((LAYERS * 16 * 8, LANES), F32),
            pltpu.VMEM((LAYERS * 32 * 8, LANES), F32),
            pltpu.VMEM((LAYERS * 8, LANES), F32),
            pltpu.VMEM((64 * 8, LANES), F32),
            pltpu.VMEM((LAYERS, 64 * 8, LANES), F32),
            pltpu.VMEM((LAYERS, 64 * 8, LANES), F32),
            pltpu.VMEM((64 * 8, LANES), F32),
            pltpu.VMEM((512, 256), F32),
            pltpu.VMEM((512, 256), F32),
            pltpu.SemaphoreType.DMA((2,)),
            pltpu.SemaphoreType.DMA((2,)),
            pltpu.SemaphoreType.DMA,
            pltpu.SemaphoreType.DMA,
            pltpu.SemaphoreType.DMA,
            pltpu.SemaphoreType.DMA((len(STAGES),)),
        ],
        compiler_params=pltpu.CompilerParams(
            collective_id=0, has_side_effects=True, vmem_limit_bytes=60 * 1024 * 1024
        ),
        name="cycle",
    )(
        grid_cells,
        visibilities,
        weights.reshape(1, VIS_DEV),
        layer_index.reshape(1, VIS_DEV),
        group_index.reshape(1, VIS_DEV),
        plane_depths,
    )
    return dirty[None] - sky_model


def solution(mesh):
    both = ("wa", "ch")
    return jax.shard_map(
        on_device,
        mesh=mesh,
        in_specs=(
            P(None, both),
            P(None, both),
            P(both),
            P(both),
            P(both),
            P("wa"),
            P("ch", "wa", None),
        ),
        out_specs=P("ch", "wa", None),
        check_vma=False,
    )
```

```python
import functools
import math

import jax
import jax.numpy as jnp
from jax import lax
from jax.experimental import pallas as pl
from jax.experimental.pallas import tpu as pltpu
from jax.sharding import PartitionSpec as P

F32 = jnp.float32
BF16 = jnp.bfloat16
I32 = jnp.int32

GRID = 8192
LAYERS = 32
GROUPS = 4
SOURCES = 128
CAP = 8
LANES = 128
VIS_DEV = 512
ROWS = 16
COLS = 4096
BLOCKS = COLS // 256
ALL = SOURCES - 1
FAR_FIRST = (2, 1, 3, 0)
STAGES = ((0, 0), (0, 1), (1, 0), (3, 0), (1, 1), (3, 1), (2, 0), (2, 1))

SIN_C = (4.442867903034145, -7.307443421379447, 3.5947880792825875, -0.7843740327506916)
COS_C = (1.4142134962552289, -6.978850948563853, 5.7394603769076955, -1.8835579059892091, 0.31068802753070307)


def horner(g, coefs):
    total = coefs[-1] * g + coefs[-2]
    for c in coefs[-3::-1]:
        total = total * g + c
    return total


def sincos_turns(f):
    g = f * f
    s = horner(g, SIN_C) * f
    c = horner(g, COS_C)
    return 1.0 - s * s, s * c


def half_turns(f):
    g = f * f
    return horner(g, SIN_C) * f, horner(g, COS_C)


def csquare(a):
    return a[0] * a[0] - a[1] * a[1], 2.0 * (a[0] * a[1])


def sincos_phase(p):
    q = ((p + GRID) & (2 * GRID - 1)) - GRID
    return sincos_turns(q.astype(F32) * (1.0 / (2 * GRID)))


def cmul(a, b):
    return a[0] * b[0] - a[1] * b[1], a[0] * b[1] + a[1] * b[0]


def fill_blocks(cells, vis, weights, layer, group, blocks, notes):
    w = weights[...]
    target_row = (layer[...] * GROUPS + group[...]).astype(F32)
    pieces = VIS_DEV // LANES
    lane = lax.broadcasted_iota(I32, (LANES, LANES), 1)
    sub = lax.broadcasted_iota(I32, (LANES, LANES), 0)
    slots = []
    for b in range(pieces):
        mine = target_row[:, b * LANES : (b + 1) * LANES]
        across = jnp.broadcast_to(mine, (LANES, LANES)).T
        hits = jnp.where((across == mine) & (lane < sub), 1.0, 0.0)
        for other in range(b):
            theirs = target_row[:, other * LANES : (other + 1) * LANES]
            hits += jnp.where(across == theirs, 1.0, 0.0)
        rank = jnp.sum(hits, axis=1, keepdims=True).astype(I32)
        t = across.astype(I32)
        slots.append((t & 3) * (LAYERS * CAP) + (t >> 2) * CAP + rank)
    zero = jnp.zeros((1, VIS_DEV), F32)
    values = jnp.concatenate(
        [
            w * vis[0:1, :],
            w * vis[1:2, :],
            cells[0:1, :].astype(F32),
            cells[1:2, :].astype(F32),
            zero,
            zero,
            zero,
            zero,
        ],
        0,
    )
    high = values.astype(BF16)
    rest = values - high.astype(F32)
    middle = rest.astype(BF16)
    low = (rest - middle.astype(F32)).astype(BF16)
    for group_number in range(GROUPS):
        for half in range(2):
            first = (group_number * 2 + half) * LANES
            picks = jnp.concatenate(
                [jnp.where(slots[b] == lane + first, 1.0, 0.0).astype(BF16) for b in range(pieces)], 0
            )
            total = jnp.dot(high, picks, preferred_element_type=F32)
            total += jnp.dot(middle, picks, preferred_element_type=F32)
            total += jnp.dot(low, picks, preferred_element_type=F32)
            blocks[group_number, half] = total[0:4]
        power = jnp.sum(jnp.where(group[...] == group_number, w * w, 0.0), axis=1, keepdims=True)
        notes[group_number] = jnp.zeros((1, LANES), F32) + power


def kernel(
    cells_hbm, vis_hbm, weights_hbm, layer_hbm, group_hbm, depth_hbm, out,
    cells, vis, weights, layer, group, depth, load_sem,
    blocks, notes, recv, heard, mydepth, depths, vals, wtab, ltab, ntab, c8, dterm, stab, ctab, acc, x_a, x_b,
    send_sem, recv_sem, note_send, note_recv, depth_send, depth_recv,
):
    wa = lax.axis_index("wa")
    ch = lax.axis_index("ch")
    me = wa * GROUPS + ch
    row0 = wa * ROWS
    loads = [
        pltpu.make_async_copy(src, dst, load_sem.at[i])
        for i, (src, dst) in enumerate(
            (
                (cells_hbm, cells),
                (vis_hbm, vis),
                (weights_hbm, weights),
                (layer_hbm, layer),
                (group_hbm, group),
                (depth_hbm, depth),
            )
        )
    ]
    for load in loads:
        load.start()
    barrier = pltpu.get_barrier_semaphore()
    mesh_id = pl.DeviceIdType.MESH

    x, zy = wa // 8, lax.rem(wa, 8)
    z, y = zy // 4, lax.rem(zy, 4)

    def moved(dx, dz, dy):
        return lax.rem(x + dx, 4) * 8 + lax.rem(z + dz, 2) * 4 + lax.rem(y + dy, 4)

    def each_peer(act):
        for dx in FAR_FIRST:
            for dz in (1, 0):
                for dy in FAR_FIRST:
                    if dx or dz or dy:
                        to = moved(dx, dz, dy)
                        for c in range(GROUPS):
                            act(to, c)
        for i in range(1, GROUPS):
            act(wa, lax.rem(ch + i, GROUPS))

    def greet(w, c):
        pl.semaphore_signal(barrier, inc=1, device_id=(w, c), device_id_type=mesh_id)

    each_peer(greet)
    for load in loads:
        load.wait()
    mydepth[0] = jnp.zeros((1, LANES), F32) + depth[0]
    fill_blocks(cells, vis, weights, layer, group, blocks, notes)
    sub = lax.broadcasted_iota(I32, (8, LANES), 0)
    lane = lax.broadcasted_iota(I32, (8, LANES), 1)
    for sl in range(2):
        rows = (row0 + 768) + (8 + sub if sl == 0 else 7 - sub)
        l = 0.8 * rows.astype(F32) / GRID
        for sn in range(2):
            for c0 in range(BLOCKS):
                cols = 256 * c0 - 1024 + (128 + lane if sn == 0 else 127 - lane)
                m = 0.8 * cols.astype(F32) / GRID
                q = l * l + m * m
                t = (c0 * 2 + sl) * 2 + sn
                dterm[t * 8 : t * 8 + 8, :] = -q / (1.0 + jnp.sqrt(1.0 - q))
    acc[...] = jnp.zeros_like(acc)
    x_b[...] = jnp.zeros_like(x_b)
    pl.semaphore_wait(barrier, ALL)

    for i, (dx, dz) in enumerate(STAGES):
        for dy in range(4):
            if dx or dz or dy:
                to = moved(dx, dz, dy)
                pltpu.make_async_remote_copy(
                    src_ref=mydepth.at[0], dst_ref=depths.at[wa],
                    send_sem=depth_send, recv_sem=depth_recv.at[i],
                    device_id=(to, lax.rem(ch + 2 * dz, GROUPS)), device_id_type=mesh_id,
                ).start()
    for half in range(2):

        def send(w, c):
            pltpu.make_async_remote_copy(
                src_ref=blocks.at[c, half], dst_ref=recv.at[half, me],
                send_sem=send_sem.at[half], recv_sem=recv_sem.at[half],
                device_id=(w, c), device_id_type=mesh_id,
            ).start()

        each_peer(send)

    def send_note(w, c):
        pltpu.make_async_remote_copy(
            src_ref=notes.at[c], dst_ref=heard.at[me], send_sem=note_send, recv_sem=note_recv,
            device_id=(w, c), device_id_type=mesh_id,
        ).start()

    each_peer(send_note)
    for half in range(2):
        recv[half, me] = blocks[ch, half]
    heard[me] = notes[ch]
    depths[wa] = mydepth[0]

    for i, (dx, dz) in enumerate(STAGES):
        some = depths.at[pl.ds(0, 4 if i else 3)]
        pltpu.make_async_copy(some, some, depth_recv.at[i]).wait()
        first = lax.rem(x + (4 - dx), 4) * 8 + lax.rem(z + dz, 2) * 4

        def screens(n, carry):
            j = first + n
            w = depths[j]
            for p in range(64):
                t = w * dterm[p * 8 : p * 8 + 8, :]
                s, c = half_turns(t - jnp.round(t))
                stab[j, p * 8 : p * 8 + 8, :] = s
                ctab[j, p * 8 : p * 8 + 8, :] = c
            return carry

        lax.fori_loop(0, 4, screens, 0)

    def tables(jc, carry):
        base = pl.multiple_of(jc * 32, 32)
        zr = vals[0, pl.ds(base, 32), :]
        zi = vals[1, pl.ds(base, 32), :]
        u = vals[2, pl.ds(base, 32), :].astype(I32)
        v = vals[3, pl.ds(base, 32), :].astype(I32)

        def put(ref, per_layer, q, x):
            for i in range(4):
                at = pl.multiple_of((jc * 4 + i) * per_layer * 8, 8) + q * 8
                ref[pl.ds(at, 8), :] = x[i * 8 : i * 8 + 8]

        w = cmul((zr, zi), sincos_phase((2 * row0 + 1551) * u - 1793 * v))
        step = sincos_phase(512 * v)
        last, w = w, cmul(w, step)
        put(wtab, 32, 0, last[0])
        put(wtab, 32, 1, last[1])
        twice = step[0] + step[0]
        for c0 in range(1, BLOCKS):
            put(wtab, 32, c0 * 2, w[0])
            put(wtab, 32, c0 * 2 + 1, w[1])
            if c0 + 1 < BLOCKS:
                last, w = w, (twice * w[0] - last[0], twice * w[1] - last[1])
        e = sincos_phase(u)
        last = e[0], -e[1]
        twice = 2.0 - 4.0 * (e[1] * e[1])
        for n in range(8):
            put(ltab, 16, n, e[0])
            put(ltab, 16, 8 + n, e[1])
            if n < 7:
                last, e = e, (twice * e[0] - last[0], twice * e[1] - last[1])
        e = sincos_phase(v)
        step = csquare(e)
        last = e[0], -e[1]
        twice = step[0] + step[0]
        eighth = csquare(csquare(csquare(step)))
        for n in range(8):
            put(ntab, 32, n, e[0])
            put(ntab, 32, 15 - n, e[0])
            put(ntab, 32, 16 + n, e[1])
            put(ntab, 32, 31 - n, e[1])
            if n < 7:
                last, e = e, (twice * e[0] - last[0], twice * e[1] - last[1])
        c8[pl.ds(base, 32), :] = 2.0 * eighth[0]
        return carry

    def expand(j, lhs, rhs):
        for s in range(8):
            ks = slice(s * LANES, (s + 1) * LANES)
            lbase = ltab[pl.ds(j * 128 + s, 16, stride=8), :]
            for q in range(32):
                row = wtab[pl.ds(j * 256 + q * 8 + s, 1), :]
                lhs[q * 16 : q * 16 + 16, ks] = (lbase * row).astype(BF16)
            c2 = c8[pl.ds(j * 8 + s, 1), :]
            for part in range(2):
                low = ntab[pl.ds(j * 256 + part * 128 + s, 8, stride=8), :]
                back = ntab[pl.ds(j * 256 + part * 128 + 64 + s, 8, stride=8), :]
                high = c2 * low - back if part == 0 else c2 * low + back
                for b in range(8):
                    at = part * 128 + b * 16
                    rhs[at : at + 16, ks] = jnp.concatenate([low, high], 0).astype(BF16)
                    if b < 7:
                        low = c2 * high - low
                        high = c2 * low - high

    def multiply(ximg, lhs, rhs):
        ximg[...] = lax.dot_general(
            lhs[...], rhs[...], (((1,), (1,)), ((), ())), preferred_element_type=F32
        )

    def image(j, ximg):
        for c0 in range(BLOCKS):
            parts = []
            for ri in range(2):
                at = (c0 * 2 + ri) * 16
                cc = ximg[at : at + 8, 0:LANES]
                cs = ximg[at : at + 8, LANES:]
                sc = ximg[at + 8 : at + 16, 0:LANES]
                ss = ximg[at + 8 : at + 16, LANES:]
                parts.append((cc - ss, cc + ss, sc + cs, sc - cs))
            (ra, rb, rp, rm), (ia, ib, ip, im) = parts
            pixels = ((ra - ip, ia + rp), (rb - im, ib + rm), (rb + im, ib - rm), (ra + ip, ia - rp))
            for k, (pr, pi) in enumerate(pixels):
                at = (c0 * 4 + k) * 8
                s = stab[j, at : at + 8, :]
                c = ctab[j, at : at + 8, :]
                acc[at : at + 8, :] += pr - s * (s * pr + c * pi)

    def arrive(half):
        arriving = recv.at[half, pl.ds(0, ALL)]
        pltpu.make_async_copy(arriving, arriving, recv_sem.at[half]).wait()
        for v in range(4):
            vals[v, half * LANES : (half + 1) * LANES, :] = recv[half, :, v, :].T

    def all_layers(lhs_a, rhs_a, lhs_b, rhs_b):
        arrive(0)
        tables(0, 0)
        expand(0, lhs_a, rhs_a)

        def several(jj, carry):
            for i in range(0, 4, 2):
                j = 4 * jj + i
                multiply(x_a, lhs_a, rhs_a)
                if i == 0:
                    tables(jnp.minimum(jj + 1, LAYERS // 4 - 1), 0)
                image(jnp.maximum(j - 1, 0), x_b)
                expand(j + 1, lhs_b, rhs_b)
                multiply(x_b, lhs_b, rhs_b)
                image(j, x_a)
                expand(jnp.minimum(j + 2, LAYERS - 1), lhs_a, rhs_a)
            return carry

        lax.fori_loop(0, LAYERS // 8 - 1, several, 0)
        arrive(1)
        lax.fori_loop(LAYERS // 8 - 1, LAYERS // 4, several, 0)
        image(LAYERS - 1, x_b)

    pl.run_scoped(
        all_layers,
        pltpu.VMEM((512, 1024), BF16),
        pltpu.VMEM((256, 1024), BF16),
        pltpu.VMEM((512, 1024), BF16),
        pltpu.VMEM((256, 1024), BF16),
    )

    all_notes = heard.at[pl.ds(0, ALL)]
    pltpu.make_async_copy(all_notes, all_notes, note_recv).wait()
    noise = jnp.sum(heard[...], axis=0)
    scale = lax.rsqrt(noise)
    back_lane = (LANES - 1) - lane
    for c0 in range(BLOCKS):
        for k in range(4):
            at = (c0 * 4 + k) * 8
            tile = acc[at : at + 8, :] * scale
            if k % 2 == 1:
                tile = jnp.take_along_axis(tile, back_lane, axis=1, mode="promise_in_bounds")
            cols = slice(c0 * 256 + (128 if k % 2 == 0 else 0), c0 * 256 + (256 if k % 2 == 0 else 128))
            if k < 2:
                out[8:16, cols] = tile
            else:
                for n in range(8):
                    out[7 - n : 8 - n, cols] = tile[n : n + 1]
    pltpu.make_async_copy(all_notes, all_notes, note_send).wait()
    others = depths.at[pl.ds(0, LAYERS - 1)]
    pltpu.make_async_copy(others, others, depth_send).wait()
    for half in range(2):
        sent = recv.at[half, pl.ds(0, ALL)]
        pltpu.make_async_copy(sent, sent, send_sem.at[half]).wait()


def on_device(grid_cells, visibilities, weights, layer_index, group_index, plane_depths, sky_model):
    vmem = pl.BlockSpec(memory_space=pltpu.VMEM)
    hbm = pl.BlockSpec(memory_space=pltpu.HBM)
    dirty = pl.pallas_call(
        kernel,
        out_shape=jax.ShapeDtypeStruct((ROWS, COLS), F32),
        in_specs=[hbm] * 6,
        out_specs=vmem,
        scratch_shapes=[
            pltpu.VMEM((2, VIS_DEV), I32),
            pltpu.VMEM((2, VIS_DEV), F32),
            pltpu.VMEM((1, VIS_DEV), F32),
            pltpu.VMEM((1, VIS_DEV), I32),
            pltpu.VMEM((1, VIS_DEV), I32),
            pltpu.SMEM((1,), F32),
            pltpu.SemaphoreType.DMA((6,)),
            pltpu.VMEM((GROUPS, 2, 4, LANES), F32),
            pltpu.VMEM((GROUPS, 1, LANES), F32),
            pltpu.VMEM((2, SOURCES, 4, LANES), F32),
            pltpu.VMEM((SOURCES, 1, LANES), F32),
            pltpu.VMEM((1, 1, LANES), F32),
            pltpu.VMEM((LAYERS, 1, LANES), F32),
            pltpu.VMEM((4, LAYERS * CAP, LANES), F32),
            pltpu.VMEM((LAYERS * 32 * 8, LANES), F32),
            pltpu.VMEM((LAYERS * 16 * 8, LANES), F32),
            pltpu.VMEM((LAYERS * 32 * 8, LANES), F32),
            pltpu.VMEM((LAYERS * 8, LANES), F32),
            pltpu.VMEM((64 * 8, LANES), F32),
            pltpu.VMEM((LAYERS, 64 * 8, LANES), F32),
            pltpu.VMEM((LAYERS, 64 * 8, LANES), F32),
            pltpu.VMEM((64 * 8, LANES), F32),
            pltpu.VMEM((512, 256), F32),
            pltpu.VMEM((512, 256), F32),
            pltpu.SemaphoreType.DMA((2,)),
            pltpu.SemaphoreType.DMA((2,)),
            pltpu.SemaphoreType.DMA,
            pltpu.SemaphoreType.DMA,
            pltpu.SemaphoreType.DMA,
            pltpu.SemaphoreType.DMA((len(STAGES),)),
        ],
        compiler_params=pltpu.CompilerParams(
            collective_id=0, has_side_effects=True, vmem_limit_bytes=60 * 1024 * 1024
        ),
        name="cycle",
    )(
        grid_cells,
        visibilities,
        weights.reshape(1, VIS_DEV),
        layer_index.reshape(1, VIS_DEV),
        group_index.reshape(1, VIS_DEV),
        plane_depths,
    )
    return dirty[None] - sky_model


def solution(mesh):
    both = ("wa", "ch")
    return jax.shard_map(
        on_device,
        mesh=mesh,
        in_specs=(
            P(None, both),
            P(None, both),
            P(both),
            P(both),
            P(both),
            P("wa"),
            P("ch", "wa", None),
        ),
        out_specs=P("ch", "wa", None),
        check_vma=False,
    )
```

```python
import functools
import math

import jax
import jax.numpy as jnp
from jax import lax
from jax.experimental import pallas as pl
from jax.experimental.pallas import tpu as pltpu
from jax.sharding import PartitionSpec as P

F32 = jnp.float32
BF16 = jnp.bfloat16
I32 = jnp.int32

GRID = 8192
LAYERS = 32
GROUPS = 4
SOURCES = 128
CAP = 8
LANES = 128
VIS_DEV = 512
ROWS = 16
COLS = 4096
BLOCKS = COLS // 256
ALL = SOURCES - 1
FAR_FIRST = (2, 1, 3, 0)
HOPS = (0, 1, 2, 1)
OFFSETS = [(dx, dz, dy) for dx in range(4) for dz in range(2) for dy in range(4)]
CLASSES = [[o for o in OFFSETS if HOPS[o[0]] + o[1] + HOPS[o[2]] == h] for h in range(6)]

SIN_C = (4.442867903034145, -7.307443421379447, 3.5947880792825875, -0.7843740327506916)
COS_C = (1.4142134962552289, -6.978850948563853, 5.7394603769076955, -1.8835579059892091, 0.31068802753070307)


def horner(g, coefs):
    total = coefs[-1] * g + coefs[-2]
    for c in coefs[-3::-1]:
        total = total * g + c
    return total


def sincos_turns(f):
    g = f * f
    s = horner(g, SIN_C) * f
    c = horner(g, COS_C)
    return 1.0 - s * s, s * c


def half_turns(f):
    g = f * f
    return horner(g, SIN_C) * f, horner(g, COS_C)


def csquare(a):
    return a[0] * a[0] - a[1] * a[1], 2.0 * (a[0] * a[1])


def sincos_phase(p):
    q = ((p + GRID) & (2 * GRID - 1)) - GRID
    return sincos_turns(q.astype(F32) * (1.0 / (2 * GRID)))


def cmul(a, b):
    return a[0] * b[0] - a[1] * b[1], a[0] * b[1] + a[1] * b[0]


def fill_blocks(cells, vis, weights, layer, group, blocks, notes):
    w = weights[...]
    target_row = (layer[...] * GROUPS + group[...]).astype(F32)
    pieces = VIS_DEV // LANES
    lane = lax.broadcasted_iota(I32, (LANES, LANES), 1)
    sub = lax.broadcasted_iota(I32, (LANES, LANES), 0)
    slots = []
    for b in range(pieces):
        mine = target_row[:, b * LANES : (b + 1) * LANES]
        across = jnp.broadcast_to(mine, (LANES, LANES)).T
        hits = jnp.where((across == mine) & (lane < sub), 1.0, 0.0)
        for other in range(b):
            theirs = target_row[:, other * LANES : (other + 1) * LANES]
            hits += jnp.where(across == theirs, 1.0, 0.0)
        rank = jnp.sum(hits, axis=1, keepdims=True).astype(I32)
        t = across.astype(I32)
        slots.append((t & 3) * (LAYERS * CAP) + (t >> 2) * CAP + rank)
    zero = jnp.zeros((1, VIS_DEV), F32)
    values = jnp.concatenate(
        [
            w * vis[0:1, :],
            w * vis[1:2, :],
            cells[0:1, :].astype(F32),
            cells[1:2, :].astype(F32),
            zero,
            zero,
            zero,
            zero,
        ],
        0,
    )
    high = values.astype(BF16)
    rest = values - high.astype(F32)
    middle = rest.astype(BF16)
    low = (rest - middle.astype(F32)).astype(BF16)
    for group_number in range(GROUPS):
        for half in range(2):
            first = (group_number * 2 + half) * LANES
            picks = jnp.concatenate(
                [jnp.where(slots[b] == lane + first, 1.0, 0.0).astype(BF16) for b in range(pieces)], 0
            )
            total = jnp.dot(high, picks, preferred_element_type=F32)
            total += jnp.dot(middle, picks, preferred_element_type=F32)
            total += jnp.dot(low, picks, preferred_element_type=F32)
            blocks[group_number, half] = total[0:4]
        power = jnp.sum(jnp.where(group[...] == group_number, w * w, 0.0), axis=1, keepdims=True)
        notes[group_number] = jnp.zeros((1, LANES), F32) + power


def kernel(
    cells_hbm, vis_hbm, weights_hbm, layer_hbm, group_hbm, depth_hbm, out,
    cells, vis, weights, layer, group, depth, load_sem,
    blocks, notes, recv, heard, mydepth, depths, vals, wtab, ltab, ntab, c8, dterm, stab, ctab, acc, x_a, x_b,
    send_sem, recv_sem, note_send, note_recv, depth_send, depth_recv,
):
    wa = lax.axis_index("wa")
    ch = lax.axis_index("ch")
    me = wa * GROUPS + ch
    row0 = wa * ROWS
    loads = [
        pltpu.make_async_copy(src, dst, load_sem.at[i])
        for i, (src, dst) in enumerate(
            (
                (cells_hbm, cells),
                (vis_hbm, vis),
                (weights_hbm, weights),
                (layer_hbm, layer),
                (group_hbm, group),
                (depth_hbm, depth),
            )
        )
    ]
    for load in loads:
        load.start()
    barrier = pltpu.get_barrier_semaphore()
    mesh_id = pl.DeviceIdType.MESH

    x, zy = wa // 8, lax.rem(wa, 8)
    z, y = zy // 4, lax.rem(zy, 4)

    def moved(dx, dz, dy):
        return lax.rem(x + dx, 4) * 8 + lax.rem(z + dz, 2) * 4 + lax.rem(y + dy, 4)

    def each_peer(act):
        for dx in FAR_FIRST:
            for dz in (1, 0):
                for dy in FAR_FIRST:
                    if dx or dz or dy:
                        to = moved(dx, dz, dy)
                        for c in range(GROUPS):
                            act(to, c)
        for i in range(1, GROUPS):
            act(wa, lax.rem(ch + i, GROUPS))

    def greet(w, c):
        pl.semaphore_signal(barrier, inc=1, device_id=(w, c), device_id_type=mesh_id)

    each_peer(greet)
    for load in loads:
        load.wait()
    mydepth[0] = jnp.zeros((1, LANES), F32) + depth[0]
    fill_blocks(cells, vis, weights, layer, group, blocks, notes)
    pl.semaphore_wait(barrier, ALL)

    for i, offsets in enumerate(CLASSES):
        for dx, dz, dy in offsets:
            if i:
                pltpu.make_async_remote_copy(
                    src_ref=mydepth.at[0], dst_ref=depths.at[wa],
                    send_sem=depth_send, recv_sem=depth_recv.at[i],
                    device_id=(moved(dx, dz, dy), lax.rem(ch + 2 * dz, GROUPS)), device_id_type=mesh_id,
                ).start()
    for half in range(2):

        def send(w, c):
            pltpu.make_async_remote_copy(
                src_ref=blocks.at[c, half], dst_ref=recv.at[half, me],
                send_sem=send_sem.at[half], recv_sem=recv_sem.at[half],
                device_id=(w, c), device_id_type=mesh_id,
            ).start()

        each_peer(send)

    def send_note(w, c):
        pltpu.make_async_remote_copy(
            src_ref=notes.at[c], dst_ref=heard.at[me], send_sem=note_send, recv_sem=note_recv,
            device_id=(w, c), device_id_type=mesh_id,
        ).start()

    each_peer(send_note)
    for half in range(2):
        recv[half, me] = blocks[ch, half]
    heard[me] = notes[ch]
    depths[wa] = mydepth[0]

    sub = lax.broadcasted_iota(I32, (8, LANES), 0)
    lane = lax.broadcasted_iota(I32, (8, LANES), 1)
    for sl in range(2):
        rows = (row0 + 768) + (8 + sub if sl == 0 else 7 - sub)
        l = 0.8 * rows.astype(F32) / GRID
        for sn in range(2):
            for c0 in range(BLOCKS):
                cols = 256 * c0 - 1024 + (128 + lane if sn == 0 else 127 - lane)
                m = 0.8 * cols.astype(F32) / GRID
                q = l * l + m * m
                t = (c0 * 2 + sl) * 2 + sn
                dterm[t * 8 : t * 8 + 8, :] = -q / (1.0 + jnp.sqrt(1.0 - q))
    acc[...] = jnp.zeros_like(acc)
    x_b[...] = jnp.zeros_like(x_b)
    def screens(n, codes):
        dx, dz, dy = lax.rem(codes // 8, 4), lax.rem(codes // 4, 2), lax.rem(codes, 4)
        j = lax.rem(x + 4 - dx, 4) * 8 + lax.rem(z + dz, 2) * 4 + lax.rem(y + 4 - dy, 4)
        w = depths[j]
        for p in range(64):
            t = w * dterm[p * 8 : p * 8 + 8, :]
            s, c = half_turns(t - jnp.round(t))
            stab[j, p * 8 : p * 8 + 8, :] = s
            ctab[j, p * 8 : p * 8 + 8, :] = c
        return codes // 32

    for i, offsets in enumerate(CLASSES):
        if i:
            some = depths.at[pl.ds(0, len(offsets))]
            pltpu.make_async_copy(some, some, depth_recv.at[i]).wait()
        for at in range(0, len(offsets), 5):
            part = offsets[at : at + 5]
            codes = sum((dx * 8 + dz * 4 + dy) * 32**k for k, (dx, dz, dy) in enumerate(part))
            lax.fori_loop(0, len(part), screens, jnp.int32(codes))

    def tables(jc, carry):
        base = pl.multiple_of(jc * 32, 32)
        zr = vals[0, pl.ds(base, 32), :]
        zi = vals[1, pl.ds(base, 32), :]
        u = vals[2, pl.ds(base, 32), :].astype(I32)
        v = vals[3, pl.ds(base, 32), :].astype(I32)

        def put(ref, per_layer, q, x):
            for i in range(4):
                at = pl.multiple_of((jc * 4 + i) * per_layer * 8, 8) + q * 8
                ref[pl.ds(at, 8), :] = x[i * 8 : i * 8 + 8]

        w = cmul((zr, zi), sincos_phase((2 * row0 + 1551) * u - 1793 * v))
        step = sincos_phase(512 * v)
        last, w = w, cmul(w, step)
        put(wtab, 32, 0, last[0])
        put(wtab, 32, 1, last[1])
        twice = step[0] + step[0]
        for c0 in range(1, BLOCKS):
            put(wtab, 32, c0 * 2, w[0])
            put(wtab, 32, c0 * 2 + 1, w[1])
            if c0 + 1 < BLOCKS:
                last, w = w, (twice * w[0] - last[0], twice * w[1] - last[1])
        e = sincos_phase(u)
        last = e[0], -e[1]
        twice = 2.0 - 4.0 * (e[1] * e[1])
        for n in range(8):
            put(ltab, 16, n, e[0])
            put(ltab, 16, 8 + n, e[1])
            if n < 7:
                last, e = e, (twice * e[0] - last[0], twice * e[1] - last[1])
        e = sincos_phase(v)
        step = csquare(e)
        last = e[0], -e[1]
        twice = step[0] + step[0]
        eighth = csquare(csquare(csquare(step)))
        for n in range(8):
            put(ntab, 32, n, e[0])
            put(ntab, 32, 15 - n, e[0])
            put(ntab, 32, 16 + n, e[1])
            put(ntab, 32, 31 - n, e[1])
            if n < 7:
                last, e = e, (twice * e[0] - last[0], twice * e[1] - last[1])
        c8[pl.ds(base, 32), :] = 2.0 * eighth[0]
        return carry

    def expand(j, lhs, rhs):
        for s in range(8):
            ks = slice(s * LANES, (s + 1) * LANES)
            lbase = ltab[pl.ds(j * 128 + s, 16, stride=8), :]
            for q in range(32):
                row = wtab[pl.ds(j * 256 + q * 8 + s, 1), :]
                lhs[q * 16 : q * 16 + 16, ks] = (lbase * row).astype(BF16)
            c2 = c8[pl.ds(j * 8 + s, 1), :]
            for part in range(2):
                low = ntab[pl.ds(j * 256 + part * 128 + s, 8, stride=8), :]
                back = ntab[pl.ds(j * 256 + part * 128 + 64 + s, 8, stride=8), :]
                high = c2 * low - back if part == 0 else c2 * low + back
                for b in range(8):
                    at = part * 128 + b * 16
                    rhs[at : at + 16, ks] = jnp.concatenate([low, high], 0).astype(BF16)
                    if b < 7:
                        low = c2 * high - low
                        high = c2 * low - high

    def multiply(ximg, lhs, rhs):
        ximg[...] = lax.dot_general(
            lhs[...], rhs[...], (((1,), (1,)), ((), ())), preferred_element_type=F32
        )

    def image(j, ximg):
        for c0 in range(BLOCKS):
            parts = []
            for ri in range(2):
                at = (c0 * 2 + ri) * 16
                cc = ximg[at : at + 8, 0:LANES]
                cs = ximg[at : at + 8, LANES:]
                sc = ximg[at + 8 : at + 16, 0:LANES]
                ss = ximg[at + 8 : at + 16, LANES:]
                parts.append((cc - ss, cc + ss, sc + cs, sc - cs))
            (ra, rb, rp, rm), (ia, ib, ip, im) = parts
            pixels = ((ra - ip, ia + rp), (rb - im, ib + rm), (rb + im, ib - rm), (ra + ip, ia - rp))
            for k, (pr, pi) in enumerate(pixels):
                at = (c0 * 4 + k) * 8
                s = stab[j, at : at + 8, :]
                c = ctab[j, at : at + 8, :]
                acc[at : at + 8, :] += pr - s * (s * pr + c * pi)

    def arrive(half):
        arriving = recv.at[half, pl.ds(0, ALL)]
        pltpu.make_async_copy(arriving, arriving, recv_sem.at[half]).wait()
        for v in range(4):
            vals[v, half * LANES : (half + 1) * LANES, :] = recv[half, :, v, :].T

    def all_layers(lhs_a, rhs_a, lhs_b, rhs_b):
        arrive(0)
        tables(0, 0)
        expand(0, lhs_a, rhs_a)

        def several(jj, carry):
            for i in range(0, 4, 2):
                j = 4 * jj + i
                multiply(x_a, lhs_a, rhs_a)
                if i == 0:
                    tables(jnp.minimum(jj + 1, LAYERS // 4 - 1), 0)
                image(jnp.maximum(j - 1, 0), x_b)
                expand(j + 1, lhs_b, rhs_b)
                multiply(x_b, lhs_b, rhs_b)
                image(j, x_a)
                expand(jnp.minimum(j + 2, LAYERS - 1), lhs_a, rhs_a)
            return carry

        lax.fori_loop(0, LAYERS // 8 - 1, several, 0)
        arrive(1)
        lax.fori_loop(LAYERS // 8 - 1, LAYERS // 4, several, 0)
        image(LAYERS - 1, x_b)

    pl.run_scoped(
        all_layers,
        pltpu.VMEM((512, 1024), BF16),
        pltpu.VMEM((256, 1024), BF16),
        pltpu.VMEM((512, 1024), BF16),
        pltpu.VMEM((256, 1024), BF16),
    )

    all_notes = heard.at[pl.ds(0, ALL)]
    pltpu.make_async_copy(all_notes, all_notes, note_recv).wait()
    noise = jnp.sum(heard[...], axis=0)
    scale = lax.rsqrt(noise)
    back_lane = (LANES - 1) - lane
    for c0 in range(BLOCKS):
        for k in range(4):
            at = (c0 * 4 + k) * 8
            tile = acc[at : at + 8, :] * scale
            if k % 2 == 1:
                tile = jnp.take_along_axis(tile, back_lane, axis=1, mode="promise_in_bounds")
            cols = slice(c0 * 256 + (128 if k % 2 == 0 else 0), c0 * 256 + (256 if k % 2 == 0 else 128))
            if k < 2:
                out[8:16, cols] = tile
            else:
                for n in range(8):
                    out[7 - n : 8 - n, cols] = tile[n : n + 1]
    pltpu.make_async_copy(all_notes, all_notes, note_send).wait()
    others = depths.at[pl.ds(0, LAYERS - 1)]
    pltpu.make_async_copy(others, others, depth_send).wait()
    for half in range(2):
        sent = recv.at[half, pl.ds(0, ALL)]
        pltpu.make_async_copy(sent, sent, send_sem.at[half]).wait()


def on_device(grid_cells, visibilities, weights, layer_index, group_index, plane_depths, sky_model):
    vmem = pl.BlockSpec(memory_space=pltpu.VMEM)
    hbm = pl.BlockSpec(memory_space=pltpu.HBM)
    dirty = pl.pallas_call(
        kernel,
        out_shape=jax.ShapeDtypeStruct((ROWS, COLS), F32),
        in_specs=[hbm] * 6,
        out_specs=vmem,
        scratch_shapes=[
            pltpu.VMEM((2, VIS_DEV), I32),
            pltpu.VMEM((2, VIS_DEV), F32),
            pltpu.VMEM((1, VIS_DEV), F32),
            pltpu.VMEM((1, VIS_DEV), I32),
            pltpu.VMEM((1, VIS_DEV), I32),
            pltpu.SMEM((1,), F32),
            pltpu.SemaphoreType.DMA((6,)),
            pltpu.VMEM((GROUPS, 2, 4, LANES), F32),
            pltpu.VMEM((GROUPS, 1, LANES), F32),
            pltpu.VMEM((2, SOURCES, 4, LANES), F32),
            pltpu.VMEM((SOURCES, 1, LANES), F32),
            pltpu.VMEM((1, 1, LANES), F32),
            pltpu.VMEM((LAYERS, 1, LANES), F32),
            pltpu.VMEM((4, LAYERS * CAP, LANES), F32),
            pltpu.VMEM((LAYERS * 32 * 8, LANES), F32),
            pltpu.VMEM((LAYERS * 16 * 8, LANES), F32),
            pltpu.VMEM((LAYERS * 32 * 8, LANES), F32),
            pltpu.VMEM((LAYERS * 8, LANES), F32),
            pltpu.VMEM((64 * 8, LANES), F32),
            pltpu.VMEM((LAYERS, 64 * 8, LANES), F32),
            pltpu.VMEM((LAYERS, 64 * 8, LANES), F32),
            pltpu.VMEM((64 * 8, LANES), F32),
            pltpu.VMEM((512, 256), F32),
            pltpu.VMEM((512, 256), F32),
            pltpu.SemaphoreType.DMA((2,)),
            pltpu.SemaphoreType.DMA((2,)),
            pltpu.SemaphoreType.DMA,
            pltpu.SemaphoreType.DMA,
            pltpu.SemaphoreType.DMA,
            pltpu.SemaphoreType.DMA((len(CLASSES),)),
        ],
        compiler_params=pltpu.CompilerParams(
            collective_id=0, has_side_effects=True, vmem_limit_bytes=60 * 1024 * 1024
        ),
        name="cycle",
    )(
        grid_cells,
        visibilities,
        weights.reshape(1, VIS_DEV),
        layer_index.reshape(1, VIS_DEV),
        group_index.reshape(1, VIS_DEV),
        plane_depths,
    )
    return dirty[None] - sky_model


def solution(mesh):
    both = ("wa", "ch")
    return jax.shard_map(
        on_device,
        mesh=mesh,
        in_specs=(
            P(None, both),
            P(None, both),
            P(both),
            P(both),
            P(both),
            P("wa"),
            P("ch", "wa", None),
        ),
        out_specs=P("ch", "wa", None),
        check_vma=False,
    )
```
